256 devices in a mesh: expert: 8 (over z), tp: 32 (over x, y, core).
Axes of the slice: x: 4, y: 4, z: 8, core: 2. Of those that a mesh axis runs over, the one named last changes fastest.
Arguments:
- tokens: bfloat16 [1024, 4096], P('expert', 'tp'), may hold values from -6 to 6
- norm_gain: bfloat16 [4096], replicated, may hold values from 0.5 to 1.5
- route_logits: float32 [1024, 2], P('expert'), may hold values from -6 to 6
- expert_ids: int32 [1024, 2], P('expert'), may hold values from 0 to 7, all different within a row; in each aligned block of 128 rows (0 to 127, 128 to 255, ...) at most 64 rows name the same one
- active: int32 [1024], P('expert'), may hold values 0 or 1
- gate_weight: bfloat16 [8, 14336, 4096], P('expert', 'tp'), may hold values from -0.09375 to 0.09375
- up_weight: bfloat16 [8, 14336, 4096], P('expert', 'tp'), may hold values from -0.09375 to 0.09375
- down_weight: bfloat16 [8, 14336, 4096], P('expert', 'tp'), may hold values from -0.046875 to 0.046875
Outputs:
- mixed: bfloat16 [1024, 4096], P('expert', 'tp')
The draws below stay inside these ranges and needn't reach their ends.
Inputs may be any that keep to these rules, and one draw needn't show every extreme that they name: `expert_ids`: each token names 2 different experts. In each block of 128 consecutive token slots (the slots of one index of expert) no expert is named by more than 64 tokens, a bound that some block reaches. `active`: each entry is 0 or 1.
All inputs are finite; a program needn't handle non-finite values.
Results may differ from the reference program's by a relative error of at most 0.0025.
Values may be sent and summed in bfloat16 or wider, within the bound.
A program may use at most 64 MiB of HBM per device.

```python
import math
import jax
import jax.numpy as jnp
import numpy as np
from jax import lax

D = 4096
FF = 14336
TOP = 2
WORDS_PER_GROUP = 128
EXPERTS = 8
TOKENS = 1024
CAP = 64


def with_ends(result, rng, low, high):
    extent = result.shape
    place = [jax.random.randint(jax.random.fold_in(rng, axis), (), 0, extent[axis]) for axis in range(len(extent))]
    result = result.at[tuple(place)].set(low)
    longest = extent.index(max(extent))
    place[longest] = (place[longest] + 1) % extent[longest]
    return result.at[tuple(place)].set(high)


def strengthened(array, rng, source, target, blocks, factor):
    def block_of(axis_at):
        return (jnp.arange(array.shape[axis_at]) // (array.shape[axis_at] // blocks)).reshape((-1,) + (1,) * (array.ndim - 1 - axis_at))

    first = jax.random.permutation(rng, blocks)[block_of(target)]
    other_side = (block_of(target) + blocks // 2) % blocks
    return jnp.where((block_of(source) == first) | (block_of(source) == other_side), factor * array, array)


def steps_of(own_key, dims, cuts, smallest, high):
    factor_of = 1.0
    for axis_at, blocks in cuts:
        steps = jax.random.uniform(jax.random.fold_in(jax.random.fold_in(own_key, 6), axis_at), (blocks,), jnp.float32, smallest / len(cuts), high / len(cuts))
        factor_of = factor_of * jnp.repeat(jnp.exp(steps), dims[axis_at] // blocks).reshape((-1,) + (1,) * (len(dims) - 1 - axis_at))
    return factor_of


def deal_out(rng, own, number, rows, amount, top, most, slope):
    ranking = jax.random.permutation(rng, amount)
    heavy_load, ordinary = load_shares(amount, rows * top, most, slope, True), load_shares(amount, rows * top, most, slope, False)
    places = jnp.arange(amount)

    def named(lengths, turn):
        used = int((lengths > 0).sum())
        fixed = max(1, used // 4)
        moved = fixed + (places - fixed + turn * (used - fixed)) % max(1, amount - fixed)
        return jnp.zeros((amount,), jnp.int32).at[ranking[jnp.where(places < fixed, places, moved)]].set(jnp.asarray(lengths, jnp.int32))

    lengths = jnp.where(number % 4 == 0, named(heavy_load, number // 4), named(ordinary, number - number // 4 - 1))
    mixed = jax.random.permutation(jax.random.fold_in(own, 3), amount)
    donor, receiver = mixed[0:amount // 2 * 2:2], mixed[1:amount // 2 * 2:2]
    slack = jnp.minimum(lengths[donor] - 1, most - lengths[receiver]) // 2
    slack = jnp.where((donor == ranking[0]) | (receiver == ranking[0]) | (lengths[receiver] == 0), 0, jnp.maximum(slack, 0))
    moved = jax.random.randint(jax.random.fold_in(own, 4), (amount // 2,), 0, 1 << 20) % (slack + 1)
    lengths = lengths.at[donor].add(-moved).at[receiver].add(moved)
    members = jnp.searchsorted(jnp.cumsum(lengths), jnp.arange(rows * top), side="right").astype(jnp.int32)
    grid = members.reshape(top, rows).T
    grid = grid[jax.random.permutation(jax.random.fold_in(own, 1), rows)]
    turn = jax.random.randint(jax.random.fold_in(own, 2), (rows, 1), 0, top)
    return jnp.take_along_axis(grid, (jnp.arange(top)[None, :] + turn) % top, axis=1)


def load_shares(amount, total, bound, lean, full):
    portions = [(1 << 20) // math.isqrt(standing ** lean) + 1 for standing in range(1, amount + 1)]
    largest = bound if full else min(bound, max(-(-total // amount), total * portions[0] // sum(portions)))
    least = 1 if total - largest >= amount - 1 else 0
    holding, surplus = [largest] + [least] * (amount - 1), total - largest - least * (amount - 1)
    while surplus > 0:
        candidates = [i for i in range(1, amount) if holding[i] < largest] or [i for i in range(1, amount) if holding[i] < bound]
        mass, left = sum([portions[i] for i in candidates]), surplus
        for i in candidates:
            addition = min(bound - holding[i], max(1, left * portions[i] // mass), surplus)
            holding[i] = holding[i] + addition
            surplus = surplus - addition
    return np.array(holding)


def noise(rng, dims, width, reach, pieces=(), held_as=jnp.bfloat16):
    array = width * jax.random.normal(rng, dims, jnp.float32)
    if pieces:
        array = array * steps_of(rng, dims, pieces, -0.22, 0.18)
    return jnp.clip(array, -reach, reach).astype(held_as)


def bell_draw_with(rng, shape, spread, reach, cuts, heavy, held_as=jnp.bfloat16):
    values = spread * jax.random.normal(rng, shape, jnp.float32)
    if cuts:
        values = values * steps_of(rng, shape, cuts, -0.22, 0.18)
    return jnp.clip(strengthened(values, jax.random.fold_in(rng, 3), *heavy), -reach, reach).astype(held_as)


def setup_inputs(seed: int = 0) -> dict:
    streams_of = jax.random.split(jax.random.key(seed), 9)
    tokens = bell_draw_with(streams_of[0], (TOKENS, D), 1.0, 6.0, ((0, 8), (1, 32)), (1, 0, 32, 2.75))
    norm_gain = jnp.clip(1.0 + 0.1 * jax.random.normal(streams_of[1], (D,), jnp.float32), 0.5, 1.5).astype(jnp.bfloat16)
    route_logits = noise(streams_of[2], (TOKENS, TOP), 1.0, 6.0, ((0, 8),), jnp.float32)
    expert_ids_keys = jax.random.split(jax.random.fold_in(streams_of[3], 1), TOKENS // WORDS_PER_GROUP)
    expert_ids_turns = jax.random.permutation(jax.random.fold_in(streams_of[3], 3), TOKENS // WORDS_PER_GROUP)
    expert_ids = jax.vmap(lambda own, number: deal_out(jax.random.fold_in(streams_of[3], 2), own, number, WORDS_PER_GROUP, EXPERTS, TOP, CAP, 2))(expert_ids_keys, expert_ids_turns).reshape((TOKENS, TOP))
    active = with_ends((jax.random.randint(streams_of[4], (TOKENS,), 0, 4) < 3).astype(jnp.int32), jax.random.fold_in(streams_of[4], 1), 0, 1)
    gate_weight = noise(streams_of[5], (EXPERTS, FF, D), D ** -0.5, 0.09375, ((0, 8), (1, 32)))
    up_weight = noise(streams_of[6], (EXPERTS, FF, D), D ** -0.5, 0.09375, ((0, 8), (1, 32)))
    down_weight = noise(streams_of[7], (EXPERTS, FF, D), FF ** -0.5, 0.046875, ((0, 8), (1, 32)))
    return dict(tokens=tokens, norm_gain=norm_gain, route_logits=route_logits, expert_ids=expert_ids, active=active, gate_weight=gate_weight, up_weight=up_weight, down_weight=down_weight)


epsilon = 1e-05

def reference(tokens, norm_gain, route_logits, expert_ids, active, gate_weight, up_weight, down_weight):
    widened = tokens.astype(jnp.float32)
    mean_square = lax.optimization_barrier(jnp.sum(widened * widened, axis=1, keepdims=True)) / D
    normed = (widened * lax.rsqrt(mean_square + epsilon) * norm_gain.astype(jnp.float32)).astype(jnp.bfloat16)
    route_probs = jax.nn.softmax(route_logits, axis=1) * active.astype(jnp.float32)[:, None]

    def expert_step(combined, inputs):
        specialist_number, gate_rows, up_rows, down_rows = inputs
        gate_sum = jnp.dot(normed, gate_rows.T, preferred_element_type=jnp.float32)
        up_sum = jnp.dot(normed, up_rows.T, preferred_element_type=jnp.float32)
        inner_width = (jax.nn.silu(gate_sum) * up_sum).astype(jnp.bfloat16)
        output = jnp.dot(inner_width, down_rows, preferred_element_type=jnp.float32).astype(jnp.bfloat16)
        weight = lax.optimization_barrier(jnp.sum(jnp.where(expert_ids == specialist_number, route_probs, jnp.zeros_like(route_probs)), axis=1))
        return (combined + weight[:, None] * output.astype(jnp.float32), None)
    start_value = jnp.zeros(tokens.shape, jnp.float32)
    expert_list = jnp.arange(EXPERTS, dtype=jnp.int32)
    combined, _ = lax.scan(expert_step, start_value, (expert_list, gate_weight, up_weight, down_weight))
    return combined.astype(jnp.bfloat16)
```

```python
import jax
import jax.numpy as jnp
from jax import lax
from jax.experimental import pallas as pl
from jax.experimental.pallas import tpu as pltpu
from jax.sharding import Mesh
from jax.sharding import PartitionSpec as P

MESH = pl.DeviceIdType.MESH
EPS = 1e-05
ZS = 8
SIDE = 4
SEATS = 64
ROWS = ZS * SEATS
HALF = ROWS // 2
FEAT = 128
HID = 448
WIDTH = 4096
QROWS = HALF + 16
QMAX = 32000.0

ORDER = [(0, 0), (3, 0), (1, 0), (0, 3), (0, 1), (2, 0), (3, 3), (3, 1), (1, 3), (1, 1), (0, 2), (2, 3), (2, 1), (3, 2), (1, 2), (2, 2)]
PRODUCTS = {6: ((0, 1), (3, 2)), 8: ((4, 6),), 9: ((7, 8),), 11: ((9, 5),), 14: ((10, 11), (13, 12)), 15: ((14, 15),)}


def encode(v, ref):
    top = jnp.maximum(jnp.max(jnp.abs(v), axis=0, keepdims=True), 1e-30)
    exponent = jnp.ceil(jnp.log2(top))
    power = jnp.exp2(exponent)
    mantissa = jnp.ceil(top / power * QMAX)
    inverse = (QMAX * QMAX) / (mantissa * power)
    ref[0:HALF, :] = jnp.round(v * inverse).astype(jnp.int32).astype(jnp.int16)
    row = lax.broadcasted_iota(jnp.int32, (16, FEAT), 0)
    scale = jnp.where(row < 8, exponent.astype(jnp.int32), mantissa.astype(jnp.int32))
    ref[HALF:QROWS, :] = scale.astype(jnp.int16)


def decode(ref):
    scale = ref[HALF:QROWS, :].astype(jnp.int32).astype(jnp.float32)
    factor = scale[8:9, :] * jnp.exp2(scale[0:1, :]) * (1.0 / (QMAX * QMAX))
    return ref[0:HALF, :].astype(jnp.int32).astype(jnp.float32) * factor


def column(row):
    return jnp.broadcast_to(row, (FEAT, FEAT)).T


def dot(a, b, dims, precision=None):
    return lax.dot_general(a, b, (dims, ((), ())), precision=precision, preferred_element_type=jnp.float32)


def kernel(
    tok_ref, gain_ref, logit_ref, ids_ref, act_ref, wg_hbm, wu_hbm, wd_hbm, out_ref,
    wg, wu, dn, outbox, gathered, scale_rows, rsend, rrecv, turned, msb, xn, gate, up, hid, part, red,
    sfb, sdb, rfb, rdb, sfa, sda, rfa, rda, fin, ret,
    w_sem, dn_sem, dns_sem, dnr_sem, z_s, z_r, rz_s, rz_r, ms_s, ms_r, g_s, g_r, d_s, d_r, h_s, h_r,
    b_s, bf_r, bd_r, a_s, af_r, ad_r, t_s, t_r,
):
    z, x, y, c = (lax.axis_index(n) for n in ("expert", "x", "y", "c"))
    a = jnp.where(c == 0, x, y)
    b = jnp.where(c == 0, y, x)
    mate = {"c": 1 - c}
    pending = []

    def wrap(v):
        return lax.rem(v, SIDE)

    def to_a(s):
        return {"x": wrap(x + s * (1 - c)), "y": wrap(y + s * c)}

    def to_b(s):
        return {"x": wrap(x + s * c), "y": wrap(y + s * (1 - c))}

    def to_z(s):
        return {"expert": lax.rem(z + s, ZS)}

    def remote(src, dst, s_sem, r_sem, device, start=True):
        copy = pltpu.make_async_remote_copy(src_ref=src, dst_ref=dst, send_sem=s_sem, recv_sem=r_sem, device_id=device, device_id_type=MESH)
        if start:
            copy.start()
            pending.append(copy)
        return copy

    def arrived(ref, sem):
        pltpu.make_async_copy(ref, ref, sem).wait()

    loads = [pltpu.make_async_copy(wg_hbm, wg, w_sem.at[0]), pltpu.make_async_copy(wu_hbm, wu, w_sem.at[1])]
    for copy in loads:
        copy.start()

    def down_columns(aa, bb, core):
        xx = jnp.where(core == 0, aa, bb)
        yy = jnp.where(core == 0, bb, aa)
        return pl.ds(pl.multiple_of(((xx * SIDE + yy) * 2 + core) * FEAT, FEAT), FEAT)

    barrier = pltpu.get_barrier_semaphore()
    peers = [mate] + [{"x": wrap(x + s)} for s in (1, 2, 3)] + [{"y": wrap(y + s)} for s in (1, 2, 3)] + [to_z(s) for s in range(1, ZS)]
    for peer in peers:
        pl.semaphore_signal(barrier, inc=1, device_id=peer, device_id_type=MESH)

    for aa in range(SIDE):
        for bb in range(SIDE):
            pltpu.make_async_copy(wd_hbm.at[:, down_columns(aa, bb, c)], dn.at[c, bb, :, pl.ds(aa * FEAT, FEAT)], dn_sem).start()

    tok = tok_ref[...]
    wide = tok.astype(jnp.float32)
    squares = jnp.sum((wide * wide).T, axis=0, keepdims=True)
    msb[0] = squares

    seat_row = lax.broadcasted_iota(jnp.int32, (ROWS, FEAT), 0)
    expert_of = seat_row // SEATS
    seat_of = (seat_row - expert_of * SEATS).astype(jnp.float32)
    live = jnp.broadcast_to(act_ref[...], (ROWS, FEAT)) > 0
    first = (expert_of == jnp.broadcast_to(ids_ref[0:1, :], (ROWS, FEAT))) & live
    second = (expert_of == jnp.broadcast_to(ids_ref[1:2, :], (ROWS, FEAT))) & live
    named = jnp.where(first | second, 1.0, 0.0)
    before = jnp.where(lax.broadcasted_iota(jnp.int32, (FEAT, FEAT), 0) < lax.broadcasted_iota(jnp.int32, (FEAT, FEAT), 1), 1.0, 0.0)
    position = dot(named.astype(jnp.bfloat16), before.astype(jnp.bfloat16), ((1,), (0,)))
    seated = position == seat_of
    pick0 = jnp.where(first & seated, 1.0, 0.0)
    pick1 = jnp.where(second & seated, 1.0, 0.0)
    pick = (pick0 + pick1).astype(jnp.bfloat16)
    outbox[...] = dot(pick, tok, ((1,), (0,))).astype(jnp.bfloat16)

    pl.semaphore_wait(barrier, len(peers))

    remote(msb.at[0], msb.at[1], ms_s.at[0], ms_r.at[0], mate)
    me = a * SIDE + b
    for s in range(1, ZS):
        target = lax.rem(z + s, ZS)
        remote(
            outbox.at[pl.ds(pl.multiple_of(target * SEATS, SEATS), SEATS)],
            gathered.at[c, me, pl.ds(pl.multiple_of(z * SEATS, SEATS), SEATS)],
            z_s.at[s - 1], z_r.at[s - 1], to_z(s),
        )
    own_seats = pl.ds(pl.multiple_of(z * SEATS, SEATS), SEATS)
    gathered[c, me, own_seats, :] = outbox[own_seats, :]
    for aa in range(SIDE):
        for bb in range(SIDE):
            remote(wd_hbm.at[:, down_columns(aa, bb, 1 - c)], dn.at[c, bb, :, pl.ds(aa * FEAT, FEAT)], dns_sem, dnr_sem, mate)
            pending.pop()
    arrived(msb.at[1], ms_r.at[0])
    msb[2] = msb[0] + msb[1]
    for s in (1, 2, 3):
        remote(msb.at[2], msb.at[2 + s], ms_s.at[s], ms_r.at[s], {"x": wrap(x + s)})

    count = [0]

    def pass_on(i, j, half, device):
        k = wrap(a + i) * SIDE + wrap(b + j)
        ref = gathered.at[c, k, pl.ds(half * HALF, HALF)]
        n = count[0]
        count[0] += 1
        remote(ref, ref, g_s.at[n], g_r.at[k * 2 + half], device)

    def await_half(i, j, half):
        k = wrap(a + i) * SIDE + wrap(b + j)
        arrived(gathered.at[c, k, pl.ds(half * HALF, HALF)], g_r.at[k * 2 + half])

    def arrive(n):
        i, j = ORDER[n]
        if (i, j) == (0, 0):
            for s in range(1, ZS):
                arrived(gathered.at[c, me, pl.ds(0, SEATS)], z_r.at[s - 1])
            for h in (0, 1):
                pass_on(0, 0, h, to_a(1))
                pass_on(0, 0, 1 - h, to_a(3))
        elif j == 0:
            if i == 3:
                await_half(i, 0, 0)
                pass_on(i, 0, 0, to_a(1))
                await_half(i, 0, 1)
            elif i == 1:
                await_half(i, 0, 1)
                pass_on(i, 0, 1, to_a(3))
                await_half(i, 0, 0)
            else:
                await_half(i, 0, 0)
                await_half(i, 0, 1)
        elif j == 3:
            await_half(i, j, 0)
            pass_on(i, j, 0, to_b(1))
            await_half(i, j, 1)
        elif j == 1:
            await_half(i, j, 1)
            pass_on(i, j, 1, to_b(3))
            await_half(i, j, 0)
        else:
            await_half(i, j, 0)
            await_half(i, j, 1)
        if j == 0:
            for h in (0, 1):
                pass_on(i, 0, h, to_b(1))
                pass_on(i, 0, 1 - h, to_b(3))
        k = wrap(a + i) * SIDE + wrap(b + j)
        remote(gathered.at[c, k], gathered.at[c, k], d_s.at[n], d_r.at[k], mate)

    def product(group, opening):
        offsets = []
        for p, n in enumerate(group):
            i, j = ORDER[n]
            aa, bb = wrap(a + i), wrap(b + j)
            mine, other = aa * SIDE + bb, bb * SIDE + aa
            arrived(gathered.at[1 - c, other], d_r.at[other])
            chip = jnp.where(c == 0, mine, other)
            gains = gain_ref[chip]
            for core in (0, 1):
                k = jnp.where(c == core, mine, other)
                raw = gathered[core, k].astype(jnp.float32)
                lanes = slice(core * FEAT, (core + 1) * FEAT)
                normed = raw * scale_rows[...] * gains[:, lanes].astype(jnp.float32)
                xn[p, :, lanes] = normed.astype(jnp.bfloat16)
            offsets.append(pl.ds(pl.multiple_of(chip * 2 * FEAT, 2 * FEAT), 2 * FEAT))
        for w, total in ((wg, gate), (wu, up)):
            terms = sum(dot(xn[p], w[:, at], ((1,), (1,))) for p, at in enumerate(offsets))
            total[...] = terms if opening else total[...] + terms

    arrived(msb.at[3], ms_r.at[1])
    arrived(msb.at[4], ms_r.at[2])
    arrived(msb.at[5], ms_r.at[3])
    msb[6] = (msb[2] + msb[3]) + (msb[4] + msb[5])
    for s in (1, 2, 3):
        remote(msb.at[6], msb.at[6 + s], ms_s.at[3 + s], ms_r.at[3 + s], {"y": wrap(y + s)})
    arrive(0)
    for s in (1, 2, 3):
        arrived(msb.at[6 + s], ms_r.at[3 + s])
    mean_square = ((msb[6] + msb[7]) + (msb[8] + msb[9])) / WIDTH
    inverse = lax.rsqrt(mean_square + EPS)
    rsend[...] = dot(jnp.broadcast_to(inverse, (8, FEAT)), pick.astype(jnp.float32), ((1,), (1,)), lax.Precision.HIGHEST)[0:1, :]
    for s in range(1, ZS):
        remote(rsend, rrecv.at[z], rz_s.at[s - 1], rz_r.at[s - 1], to_z(s))
    rrecv[z] = rsend[...]

    l0, l1 = logit_ref[0:1, :], logit_ref[1:2, :]
    high = jnp.maximum(l0, l1)
    e0, e1 = jnp.exp(l0 - high), jnp.exp(l1 - high)
    alive = act_ref[...].astype(jnp.float32)
    prob0 = column(e0 / (e0 + e1) * alive)
    prob1 = column(e1 / (e0 + e1) * alive)

    arrive(1)
    arrive(2)
    arrive(3)
    arrive(4)
    for s in range(1, ZS):
        arrived(rrecv.at[z], rz_r.at[s - 1])
    lane_block = pl.ds(pl.multiple_of(z // 2 * FEAT, FEAT), FEAT)
    seat_block = pl.ds(pl.multiple_of(z % 2 * SEATS, SEATS), SEATS)
    for g in range(ZS):
        turned[...] = column(rrecv[g, :, lane_block])
        scale_rows[g * SEATS : (g + 1) * SEATS, :] = turned[seat_block, :]
    for copy in loads:
        copy.wait()
    opening = True
    for n in range(5, 16):
        arrive(n)
        for group in PRODUCTS.get(n, ()):
            product(group, opening)
            opening = False

    quarter = ROWS // 4
    for q in range(4):
        rows = slice(q * quarter, (q + 1) * quarter)
        g = gate[rows, :]
        hid[c, rows, :] = (g / (1.0 + jnp.exp(-g)) * up[rows, :]).astype(jnp.bfloat16)
        ref = hid.at[c, pl.ds(q * quarter, quarter)]
        remote(ref, ref, h_s.at[q], h_r.at[q], mate)
    arrived(dn.at[c], dn_sem)
    arrived(dn.at[1 - c], dnr_sem)
    for q in range(4):
        arrived(hid.at[1 - c, pl.ds(q * quarter, quarter)], h_r.at[q])

    def partial(j):
        bb = wrap(b + j)
        part[j] = dot(hid[0], dn[0, bb], ((1,), (0,))) + dot(hid[1], dn[1, bb], ((1,), (0,)))

    LO, HI = slice(0, HALF), slice(HALF, ROWS)

    def lanes_of(i):
        return pl.ds(pl.multiple_of(wrap(a + i) * FEAT, FEAT), FEAT)

    ahead = (2, 3, 1, 0)
    partial(2)
    for i in ahead:
        aa = wrap(a + i)
        for d, rows, step in ((0, LO, 1), (1, HI, 3)):
            encode(part[2, rows, lanes_of(i)], sfb.at[d, aa])
            remote(sfb.at[d, aa], rfb.at[d, aa], b_s.at[0, d, aa], bf_r.at[d, aa], to_b(step))
    partial(1)
    partial(3)
    partial(0)
    for i in ahead:
        aa = wrap(a + i)
        for d, j, rows, h, step in ((0, 1, HI, 1, 1), (1, 3, LO, 0, 3)):
            encode(part[j, rows, lanes_of(i)], sdb.at[d, aa, h])
            remote(sdb.at[d, aa, h], rdb.at[d, aa, h], b_s.at[1, d, aa], bd_r.at[d, aa, h], to_b(step))
        for d, j, rows, h, step in ((0, 1, LO, 0, 1), (1, 3, HI, 1, 3)):
            arrived(rfb.at[d, aa], bf_r.at[d, aa])
            encode(part[j, rows, lanes_of(i)] + decode(rfb.at[d, aa]), sdb.at[d, aa, h])
            remote(sdb.at[d, aa, h], rdb.at[d, aa, h], b_s.at[2, d, aa], bd_r.at[d, aa, h], to_b(step))

    def finish_b(i, h):
        aa = wrap(a + i)
        rows = LO if h == 0 else HI
        arrived(rdb.at[0, aa, h], bd_r.at[0, aa, h])
        arrived(rdb.at[1, aa, h], bd_r.at[1, aa, h])
        return part[0, rows, lanes_of(i)] + decode(rdb.at[0, aa, h]) + decode(rdb.at[1, aa, h])

    for d, step in ((0, 1), (1, 3)):
        encode(finish_b(2, d), sfa.at[d])
        remote(sfa.at[d], rfa.at[d], a_s.at[0, d], af_r.at[d], to_a(step))
    for d, i, h, step in ((0, 1, 1, 1), (1, 3, 0, 3)):
        encode(finish_b(i, h), sda.at[d, h])
        remote(sda.at[d, h], rda.at[d, h], a_s.at[1, d], ad_r.at[d, h], to_a(step))
    for d, i, h, step in ((0, 1, 0, 1), (1, 3, 1, 3)):
        value = finish_b(i, h)
        arrived(rfa.at[d], af_r.at[d])
        encode(value + decode(rfa.at[d]), sda.at[d, h])
        remote(sda.at[d, h], rda.at[d, h], a_s.at[2, d], ad_r.at[d, h], to_a(step))
    red[0] = finish_b(0, 0)
    red[1] = finish_b(0, 1)
    for h in (0, 1):
        arrived(rda.at[0, h], ad_r.at[0, h])
        arrived(rda.at[1, h], ad_r.at[1, h])
        fin[h * HALF : (h + 1) * HALF, :] = (red[h] + decode(rda.at[0, h]) + decode(rda.at[1, h])).astype(jnp.bfloat16)

    for s in range(1, ZS):
        target = lax.rem(z + s, ZS)
        remote(
            fin.at[pl.ds(pl.multiple_of(target * SEATS, SEATS), SEATS)],
            ret.at[own_seats],
            t_s.at[s - 1], t_r.at[s - 1], to_z(s),
        )
    ret[own_seats, :] = fin[own_seats, :]
    for s in range(1, ZS):
        arrived(ret.at[pl.ds(0, SEATS)], t_r.at[s - 1])
    back = ret[...]
    from0 = dot(pick0.astype(jnp.bfloat16), back, ((0,), (0,)))
    from1 = dot(pick1.astype(jnp.bfloat16), back, ((0,), (0,)))
    out_ref[...] = (prob0 * from0 + prob1 * from1).astype(jnp.bfloat16)

    for copy in pending:
        copy.wait_send()
    arrived(dn.at[c], dns_sem)


def local(tokens, norm_gain, route_logits, expert_ids, active, gate_weight, up_weight, down_weight):
    vmem = pl.BlockSpec(memory_space=pltpu.VMEM)
    hbm = pl.BlockSpec(memory_space=pl.ANY)
    bf16, f32, i16 = jnp.bfloat16, jnp.float32, jnp.int16
    dma = pltpu.SemaphoreType.DMA
    return pl.pallas_call(
        kernel,
        out_shape=jax.ShapeDtypeStruct((FEAT, FEAT), bf16),
        in_specs=[vmem] * 5 + [hbm] * 3,
        out_specs=vmem,
        scratch_shapes=[
            pltpu.VMEM((HID, WIDTH), bf16),
            pltpu.VMEM((HID, WIDTH), bf16),
            pltpu.VMEM((2, SIDE, HID, SIDE * FEAT), bf16),
            pltpu.VMEM((ROWS, FEAT), bf16),
            pltpu.VMEM((2, 16, ROWS, FEAT), bf16),
            pltpu.VMEM((ROWS, FEAT), f32),
            pltpu.VMEM((1, ROWS), f32),
            pltpu.VMEM((ZS, 1, ROWS), f32),
            pltpu.VMEM((FEAT, FEAT), f32),
            pltpu.VMEM((10, 1, FEAT), f32),
            pltpu.VMEM((2, ROWS, 2 * FEAT), bf16),
            pltpu.VMEM((ROWS, HID), f32),
            pltpu.VMEM((ROWS, HID), f32),
            pltpu.VMEM((2, ROWS, HID), bf16),
            pltpu.VMEM((SIDE, ROWS, SIDE * FEAT), f32),
            pltpu.VMEM((2, HALF, FEAT), f32),
            pltpu.VMEM((2, SIDE, QROWS, FEAT), i16),
            pltpu.VMEM((2, SIDE, 2, QROWS, FEAT), i16),
            pltpu.VMEM((2, SIDE, QROWS, FEAT), i16),
            pltpu.VMEM((2, SIDE, 2, QROWS, FEAT), i16),
            pltpu.VMEM((2, QROWS, FEAT), i16),
            pltpu.VMEM((2, 2, QROWS, FEAT), i16),
            pltpu.VMEM((2, QROWS, FEAT), i16),
            pltpu.VMEM((2, 2, QROWS, FEAT), i16),
            pltpu.VMEM((ROWS, FEAT), bf16),
            pltpu.VMEM((ROWS, FEAT), bf16),
            dma((2,)), dma, dma, dma,
            dma((ZS - 1,)), dma((ZS - 1,)), dma((ZS - 1,)), dma((ZS - 1,)),
            dma((7,)), dma((7,)),
            dma((30,)), dma((32,)), dma((16,)), dma((16,)), dma((4,)), dma((4,)),
            dma((3, 2, SIDE)), dma((2, SIDE)), dma((2, SIDE, 2)),
            dma((3, 2)), dma((2,)), dma((2, 2)),
            dma((ZS - 1,)), dma((ZS - 1,)),
        ],
        compiler_params=pltpu.CompilerParams(collective_id=0, has_side_effects=True, vmem_limit_bytes=60 * 1024 * 1024),
    )(
        tokens,
        norm_gain.reshape(16, 1, 2 * FEAT),
        route_logits.T,
        expert_ids.T,
        active.reshape(1, FEAT),
        gate_weight.reshape(HID, WIDTH),
        up_weight.reshape(HID, WIDTH),
        down_weight.reshape(HID, WIDTH),
    )


def solution(mesh):
    split = Mesh(mesh.devices.reshape(ZS, SIDE, SIDE, 2), ("expert", "x", "y", "c"))
    plane = ("x", "y", "c")
    weight = P("expert", plane, None)
    in_specs = (P("expert", plane), P(), P("expert", None), P("expert", None), P("expert"), weight, weight, weight)
    return jax.shard_map(local, mesh=split, in_specs=in_specs, out_specs=P("expert", plane), check_vma=False)
```

```python
import jax
import jax.numpy as jnp
from jax import lax
from jax.experimental import pallas as pl
from jax.experimental.pallas import tpu as pltpu
from jax.sharding import Mesh
from jax.sharding import PartitionSpec as P

MESH = pl.DeviceIdType.MESH
EPS = 1e-05
ZS = 8
SIDE = 4
SEATS = 64
ROWS = ZS * SEATS
HALF = ROWS // 2
QUARTER = HALF // 2
FEAT = 128
HID = 448
WIDTH = 4096
QMAX = 32000.0

ORDER = [(0, 0), (3, 0), (1, 0), (0, 3), (0, 1), (2, 0), (3, 3), (3, 1), (1, 3), (1, 1), (0, 2), (2, 3), (2, 1), (3, 2), (1, 2), (2, 2)]
MIRROR = [ORDER.index((j, i)) for i, j in ORDER]
PRODUCTS = ((1, 3), (2, 4), (5, 10), (0, 6), (7, 8), (9, 11), (13, 12), (14, 15))
BLOCKS = ((2, 3), (1, 0))

SCHEDULE = (
    ("arr", 0, 1), ("arr", 0, 2), ("arr", 0, 3), ("arr", 0, 4), ("arr", 1, 3), ("arr", 1, 4),
    ("arr", 1, 1), ("arr", 1, 2), ("arr", 0, 5), ("scale", 0), ("weights",), ("prod", 0, 0),
    ("scale", 1), ("arr", 0, 6), ("arr", 0, 7), ("prod", 0, 1), ("arr", 1, 5), ("prod", 1, 0),
    ("arr", 0, 8), ("arr", 0, 9), ("arr", 0, 10), ("prod", 1, 1), ("arr", 1, 10), ("prod", 0, 3),
    ("arr", 1, 6), ("arr", 1, 7), ("prod", 0, 4), ("prod", 0, 2), ("arr", 1, 8), ("arr", 1, 9),
    ("prod", 1, 2), ("arr", 0, 11), ("arr", 0, 12), ("prod", 1, 3), ("arr", 0, 13), ("prod", 1, 4),
    ("arr", 1, 11), ("arr", 1, 12), ("arr", 0, 14), ("arr", 1, 13), ("prod", 0, 5), ("arr", 1, 14),
    ("prod", 0, 6), ("arr", 0, 15), ("prod", 1, 5), ("prod", 1, 6), ("arr", 1, 15), ("prod", 0, 7),
    ("hidden", 0), ("down",), ("pre2", 0), ("prod", 1, 7), ("hidden", 1), ("pre2", 1),
    ("p2", 0), ("ahead", 0, 0), ("ahead", 0, 1), ("pd", 0, 0), ("direct", 0, 0, 0), ("direct", 0, 1, 0),
    ("pd", 0, 1), ("direct", 0, 0, 1), ("direct", 0, 1, 1), ("p2", 1), ("ahead", 1, 0), ("ahead", 1, 1),
    ("pd", 1, 0), ("direct", 1, 0, 0), ("direct", 1, 1, 0), ("pd", 1, 1), ("direct", 1, 0, 1), ("direct", 1, 1, 1),
    ("p0", 0), ("joined", 0, 0, 0), ("joined", 0, 0, 1), ("p0", 1), ("joined", 0, 1, 0), ("joined", 0, 1, 1),
    ("joined", 1, 0, 0), ("joined", 1, 0, 1), ("joined", 1, 1, 0), ("joined", 1, 1, 1), ("sum", 0, 0), ("sum", 0, 2),
    ("sum", 0, 1), ("own", 0), ("sum", 1, 0), ("sum", 1, 2), ("sum", 1, 1), ("own", 1),
    ("finish", 0), ("finish", 1),
)


def encode(values, ref):
    row = lax.broadcasted_iota(jnp.int32, (16, FEAT), 0)
    scale = jnp.zeros((16, FEAT), jnp.int32)
    for n, v in enumerate(values):
        top = jnp.maximum(jnp.max(jnp.abs(v), axis=0, keepdims=True), 1e-30)
        exponent = jnp.ceil(jnp.log2(top))
        power = jnp.exp2(exponent)
        mantissa = jnp.ceil(top / power * QMAX)
        inverse = (QMAX * QMAX) / (mantissa * power)
        ref[n * QUARTER : (n + 1) * QUARTER, :] = jnp.round(v * inverse).astype(jnp.int32).astype(jnp.int16)
        scale = jnp.where(row >= 8 * n, jnp.where(row < 8 * n + 4, exponent.astype(jnp.int32), mantissa.astype(jnp.int32)), scale)
    ref[len(values) * QUARTER :, :] = scale.astype(jnp.int16)


def decode(ref, n=0):
    scale = ref[ref.shape[0] - 16 :, :].astype(jnp.int32).astype(jnp.float32)
    factor = scale[8 * n + 4 : 8 * n + 5, :] * jnp.exp2(scale[8 * n : 8 * n + 1, :]) * (1.0 / (QMAX * QMAX))
    return ref[n * QUARTER : (n + 1) * QUARTER, :].astype(jnp.int32).astype(jnp.float32) * factor


def column(row):
    return jnp.broadcast_to(row, (FEAT, FEAT)).T


def dot(a, b, dims, precision=None):
    return lax.dot_general(a, b, (dims, ((), ())), precision=precision, preferred_element_type=jnp.float32)


def kernel(
    tok_ref, gain_ref, logit_ref, ids_ref, act_ref, wg_hbm, wu_hbm, wd_hbm, out_ref,
    wide_w, dn, outbox, gathered, scale_rows, rsend, rrecv, turned, msb, xn, sums, hid, part, red,
    sfb, sdb, rfb, rdb, sda, rda, fin, ret,
    w_sem, dn_sem, dns_sem, dnr_sem, z_s, z_r, rz_s, rz_r, ms_s, ms_r, g_s, g_r, d_s, d_r, h_s, h_r,
    bf_s, bf_r, bd_s, bd_r, ad_s, ad_r, t_s, t_r,
):
    z, x, y, c = (lax.axis_index(n) for n in ("expert", "x", "y", "c"))
    a = jnp.where(c == 0, x, y)
    b = jnp.where(c == 0, y, x)
    mate = {"c": 1 - c}

    def wrap(v):
        return lax.rem(v, SIDE)

    def to_a(s):
        return {"x": wrap(x + s * (1 - c)), "y": wrap(y + s * c)}

    def to_b(s):
        return {"x": wrap(x + s * c), "y": wrap(y + s * (1 - c))}

    def to_z(s):
        return {"expert": lax.rem(z + s, ZS)}

    def remote(src, dst, s_sem, r_sem, device):
        pltpu.make_async_remote_copy(src_ref=src, dst_ref=dst, send_sem=s_sem, recv_sem=r_sem, device_id=device, device_id_type=MESH).start()

    def arrived(ref, sem):
        pltpu.make_async_copy(ref, ref, sem).wait()

    for n, w in enumerate((wg_hbm, wu_hbm)):
        pltpu.make_async_copy(w, wide_w.at[n], w_sem).start()

    def down_columns(aa, bb, core):
        xx = jnp.where(core == 0, aa, bb)
        yy = jnp.where(core == 0, bb, aa)
        return pl.ds(pl.multiple_of(((xx * SIDE + yy) * 2 + core) * FEAT, FEAT), FEAT)

    barrier = pltpu.get_barrier_semaphore()
    peers = [mate] + [{"x": wrap(x + s)} for s in (1, 2, 3)] + [{"y": wrap(y + s)} for s in (1, 2, 3)] + [to_z(s) for s in range(1, ZS)]
    for peer in peers:
        pl.semaphore_signal(barrier, inc=1, device_id=peer, device_id_type=MESH)

    for aa in range(SIDE):
        for bb in range(SIDE):
            pltpu.make_async_copy(wd_hbm.at[:, down_columns(aa, bb, c)], dn.at[c, bb, :, pl.ds(aa * FEAT, FEAT)], dn_sem).start()

    tok = tok_ref[...]
    wide = tok.astype(jnp.float32)
    msb[0] = jnp.sum((wide * wide).T, axis=0, keepdims=True)

    seat_row = lax.broadcasted_iota(jnp.int32, (ROWS, FEAT), 0)
    expert_of = seat_row // SEATS
    seat_of = (seat_row - expert_of * SEATS).astype(jnp.float32)
    live = jnp.broadcast_to(act_ref[...], (ROWS, FEAT)) > 0
    first = (expert_of == jnp.broadcast_to(ids_ref[0:1, :], (ROWS, FEAT))) & live
    second = (expert_of == jnp.broadcast_to(ids_ref[1:2, :], (ROWS, FEAT))) & live
    named = jnp.where(first | second, 1.0, 0.0)
    before = jnp.where(lax.broadcasted_iota(jnp.int32, (FEAT, FEAT), 0) < lax.broadcasted_iota(jnp.int32, (FEAT, FEAT), 1), 1.0, 0.0)
    position = dot(named.astype(jnp.bfloat16), before.astype(jnp.bfloat16), ((1,), (0,)))
    seated = position == seat_of
    pick0 = jnp.where(first & seated, 1.0, 0.0)
    pick1 = jnp.where(second & seated, 1.0, 0.0)
    pick = (pick0 + pick1).astype(jnp.bfloat16)
    outbox[...] = dot(pick, tok, ((1,), (0,))).astype(jnp.bfloat16)

    pl.semaphore_wait(barrier, len(peers))
    remote(msb.at[0], msb.at[1], ms_s, ms_r.at[0], mate)
    me = a * SIDE + b
    my_half = z // 4
    own_seats = pl.ds(pl.multiple_of(z * SEATS, SEATS), SEATS)
    landing = gathered.at[my_half, c, me, pl.ds(pl.multiple_of(z % 4 * SEATS, SEATS), SEATS)]
    for s in (4, 5, 3, 6, 2, 7, 1):
        target = lax.rem(z + s, ZS)
        remote(outbox.at[pl.ds(pl.multiple_of(target * SEATS, SEATS), SEATS)], landing, z_s, z_r.at[my_half], to_z(s))
    pltpu.make_async_copy(outbox.at[own_seats], landing, z_r.at[my_half]).start()
    for aa in range(SIDE):
        for bb in range(SIDE):
            remote(wd_hbm.at[:, down_columns(aa, bb, 1 - c)], dn.at[c, bb, :, pl.ds(aa * FEAT, FEAT)], dns_sem, dnr_sem, mate)

    def pass_on(h, i, j, quarter, device, di, dj):
        k = wrap(a + i) * SIDE + wrap(b + j)
        ref = gathered.at[h, c, k]
        if quarter is not None:
            ref = ref.at[pl.ds(quarter * QUARTER, QUARTER)]
        remote(ref, ref, g_s, g_r.at[h, ORDER.index(((i - di) % 4, (j - dj) % 4))], device)

    def arrive(h, n):
        i, j = ORDER[n]
        k = wrap(a + i) * SIDE + wrap(b + j)
        if n == 0:
            arrived(gathered.at[h, c, k], z_r.at[h])
            pass_on(h, 0, 0, None, to_a(1), 1, 0)
            pass_on(h, 0, 0, None, to_a(3), 3, 0)
            pass_on(h, 0, 0, None, to_a(2), 2, 0)
        else:
            arrived(gathered.at[h, c, k], g_r.at[h, n])
        if j == 0:
            pass_on(h, i, j, None, to_b(1), 0, 1)
            pass_on(h, i, j, None, to_b(3), 0, 3)
        if j == 3:
            pass_on(h, i, j, 0, to_b(1), 0, 1)
        if j == 1:
            pass_on(h, i, j, 1, to_b(3), 0, 3)
        group = next(g for g, pair in enumerate(PRODUCTS) if MIRROR[n] in pair)
        remote(gathered.at[h, c, k], gathered.at[h, c, k], d_s, d_r.at[h, group], mate)

    opened = set()

    def product(h, group):
        arrived(gathered.at[h, 0, pl.ds(0, 2)], d_r.at[h, group])
        offsets = []
        for p, n in enumerate(PRODUCTS[group]):
            i, j = ORDER[n]
            aa, bb = wrap(a + i), wrap(b + j)
            mine, other = aa * SIDE + bb, bb * SIDE + aa
            chip = jnp.where(c == 0, mine, other)
            at = pl.ds(pl.multiple_of(chip * 2 * FEAT, 2 * FEAT), 2 * FEAT)
            gains = gain_ref[at].astype(jnp.float32).reshape(1, 2 * FEAT)
            for core in (0, 1):
                k = jnp.where(c == core, mine, other)
                lanes = slice(core * FEAT, (core + 1) * FEAT)
                normed = gathered[h, core, k].astype(jnp.float32) * scale_rows[h] * gains[:, lanes]
                xn[p, :, lanes] = normed.astype(jnp.bfloat16)
            offsets.append(at)
        for n in (0, 1):
            terms = sum(dot(xn[p], wide_w[n, :, at], ((1,), (1,))) for p, at in enumerate(offsets))
            sums[h, n] = sums[h, n] + terms if h in opened else terms
        opened.add(h)

    def hidden(h):
        g = sums[h, 0]
        hid[h, c] = (g / (1.0 + jnp.exp(-g)) * sums[h, 1]).astype(jnp.bfloat16)
        remote(hid.at[h, c], hid.at[h, c], h_s, h_r.at[h], mate)

    AHEAD, STEP, SIDES = 2, (1, 3), (1, 3)

    def partial(h, j, own, first):
        core = c if own else 1 - c
        terms = dot(hid[h, core], dn[core, wrap(b + j)], ((1,), (0,)))
        part[h, j] = terms if first else part[h, j] + terms

    def block(h, j, q, i):
        return part[h, j, q * QUARTER : (q + 1) * QUARTER, pl.ds(pl.multiple_of(wrap(a + i) * FEAT, FEAT), FEAT)]

    def send_ahead(h, g):
        for d in (0, 1):
            encode([block(h, AHEAD, d, i) for i in BLOCKS[g]], sfb.at[h, d, g])
            remote(sfb.at[h, d, g], rfb.at[h, d, g], bf_s, bf_r.at[h, d, g], to_b(STEP[d]))

    def send_direct(h, g, d):
        q = 1 - d
        encode([block(h, SIDES[d], q, i) for i in BLOCKS[g]], sdb.at[h, g, d, q])
        remote(sdb.at[h, g, d, q], rdb.at[h, g, d, q], bd_s, bd_r.at[h, g], to_b(STEP[d]))

    def send_joined(h, g, d):
        q = d
        arrived(rfb.at[h, d, g], bf_r.at[h, d, g])
        encode([block(h, SIDES[d], q, i) + decode(rfb.at[h, d, g], n) for n, i in enumerate(BLOCKS[g])], sdb.at[h, g, d, q])
        remote(sdb.at[h, g, d, q], rdb.at[h, g, d, q], bd_s, bd_r.at[h, g], to_b(STEP[d]))

    awaited = set()

    def summed(h, i):
        g = 0 if i in BLOCKS[0] else 1
        n = BLOCKS[g].index(i)
        if (h, g) not in awaited:
            awaited.add((h, g))
            arrived(rdb.at[h, g], bd_r.at[h, g])
        return [block(h, 0, q, i) + decode(rdb.at[h, g, 0, q], n) + decode(rdb.at[h, g, 1, q], n) for q in (0, 1)]

    def send_sum(h, n):
        i = (2, 1, 3)[n]
        encode(summed(h, i), sda.at[h, n])
        remote(sda.at[h, n], rda.at[h, n], ad_s, ad_r.at[h], to_a(i))

    def keep_sum(h):
        red[h, 0], red[h, 1] = summed(h, 0)

    def finish(h):
        arrived(rda.at[h], ad_r.at[h])
        for q in (0, 1):
            total = red[h, q] + decode(rda.at[h, 0], q) + decode(rda.at[h, 1], q) + decode(rda.at[h, 2], q)
            fin[h, q * QUARTER : (q + 1) * QUARTER, :] = total.astype(jnp.bfloat16)
        for m in range(4):
            g = h * 4 + m
            source, target = fin.at[h, pl.ds(m * SEATS, SEATS)], ret.at[own_seats]

            @pl.when(z != g)
            def _():
                remote(source, target, t_s, t_r, {"expert": g})

            @pl.when(z == g)
            def _():
                pltpu.make_async_copy(source, target, t_r).start()

    arrived(msb.at[1], ms_r.at[0])
    msb[2] = msb[0] + msb[1]
    for s in (1, 2, 3):
        remote(msb.at[2], msb.at[2 + s], ms_s, ms_r.at[1], {"x": wrap(x + s)})
    arrived(msb.at[pl.ds(3, 3)], ms_r.at[1])
    msb[6] = (msb[2] + msb[3]) + (msb[4] + msb[5])
    for s in (1, 2, 3):
        remote(msb.at[6], msb.at[6 + s], ms_s, ms_r.at[2], {"y": wrap(y + s)})
    arrive(0, 0)
    arrive(1, 0)
    arrived(msb.at[pl.ds(7, 3)], ms_r.at[2])
    mean_square = ((msb[6] + msb[7]) + (msb[8] + msb[9])) / WIDTH
    inverse = lax.rsqrt(mean_square + EPS)
    rsend[...] = dot(jnp.broadcast_to(inverse, (8, FEAT)), pick.astype(jnp.float32), ((1,), (1,)), lax.Precision.HIGHEST)[0:1, :]
    for s in range(1, ZS):
        remote(rsend, rrecv.at[z], rz_s, rz_r.at[my_half], to_z(s))
    pltpu.make_async_copy(rsend, rrecv.at[z], rz_r.at[my_half]).start()
    l0, l1 = logit_ref[0:1, :], logit_ref[1:2, :]
    high = jnp.maximum(l0, l1)
    e0, e1 = jnp.exp(l0 - high), jnp.exp(l1 - high)
    alive = act_ref[...].astype(jnp.float32)
    prob0 = column(e0 / (e0 + e1) * alive)
    prob1 = column(e1 / (e0 + e1) * alive)

    lane_block = pl.ds(pl.multiple_of(z // 2 * FEAT, FEAT), FEAT)
    seat_block = pl.ds(pl.multiple_of(z % 2 * SEATS, SEATS), SEATS)

    def scales(h):
        arrived(rrecv.at[pl.ds(0, 4)], rz_r.at[h])
        for m in range(4):
            turned[...] = column(rrecv[h * 4 + m, :, lane_block])
            scale_rows[h, m * SEATS : (m + 1) * SEATS, :] = turned[seat_block, :]

    def down_ready():
        arrived(dn.at[c], dn_sem)
        arrived(dn.at[1 - c], dnr_sem)

    def weights_ready():
        arrived(wide_w, w_sem)

    def both_cores(h):
        arrived(hid.at[h, 1 - c], h_r.at[h])
        partial(h, AHEAD, False, False)

    def whole_partial(h, j):
        partial(h, j, True, True)
        partial(h, j, False, False)

    events = {
        "arr": arrive,
        "scale": scales,
        "weights": weights_ready,
        "prod": product,
        "hidden": hidden,
        "down": down_ready,
        "pre2": lambda h: partial(h, AHEAD, True, True),
        "p2": both_cores,
        "ahead": send_ahead,
        "pd": lambda h, d: whole_partial(h, SIDES[d]),
        "direct": send_direct,
        "joined": send_joined,
        "p0": lambda h: whole_partial(h, 0),
        "sum": send_sum,
        "own": keep_sum,
        "finish": finish,
    }
    for name, *which in SCHEDULE:
        events[name](*which)
    arrived(ret, t_r)
    back = ret[...]
    from0 = dot(pick0.astype(jnp.bfloat16), back, ((0,), (0,)))
    from1 = dot(pick1.astype(jnp.bfloat16), back, ((0,), (0,)))
    out_ref[...] = (prob0 * from0 + prob1 * from1).astype(jnp.bfloat16)

    arrived(outbox.at[pl.ds(0, ROWS - SEATS)], z_s)
    arrived(rrecv.at[pl.ds(0, ZS - 1)], rz_s)
    arrived(msb.at[pl.ds(0, 7)], ms_s)
    arrived(gathered.at[:, 0, pl.ds(0, 15)], g_s)
    arrived(gathered.at[:, 0], d_s)
    arrived(hid.at[:, 0], h_s)
    arrived(sfb, bf_s)
    arrived(sdb, bd_s)
    arrived(sda, ad_s)
    arrived(ret.at[pl.ds(0, ROWS - SEATS)], t_s)
    arrived(dn.at[c], dns_sem)


def local(tokens, norm_gain, route_logits, expert_ids, active, gate_weight, up_weight, down_weight):
    vmem = pl.BlockSpec(memory_space=pltpu.VMEM)
    hbm = pl.BlockSpec(memory_space=pltpu.HBM)
    bf16, f32, i16 = jnp.bfloat16, jnp.float32, jnp.int16
    dma = pltpu.SemaphoreType.DMA
    double = 2 * QUARTER + 16
    return pl.pallas_call(
        kernel,
        out_shape=jax.ShapeDtypeStruct((FEAT, FEAT), bf16),
        in_specs=[vmem] * 5 + [hbm] * 3,
        out_specs=vmem,
        scratch_shapes=[
            pltpu.VMEM((2, HID, WIDTH), bf16),
            pltpu.VMEM((2, SIDE, HID, SIDE * FEAT), bf16),
            pltpu.VMEM((ROWS, FEAT), bf16),
            pltpu.VMEM((2, 2, 16, HALF, FEAT), bf16),
            pltpu.VMEM((2, HALF, FEAT), f32),
            pltpu.VMEM((1, ROWS), f32),
            pltpu.VMEM((ZS, 1, ROWS), f32),
            pltpu.VMEM((FEAT, FEAT), f32),
            pltpu.VMEM((10, 1, FEAT), f32),
            pltpu.VMEM((2, HALF, 2 * FEAT), bf16),
            pltpu.VMEM((2, 2, HALF, HID), f32),
            pltpu.VMEM((2, 2, HALF, HID), bf16),
            pltpu.VMEM((2, SIDE, HALF, SIDE * FEAT), f32),
            pltpu.VMEM((2, 2, QUARTER, FEAT), f32),
            pltpu.VMEM((2, 2, 2, double, FEAT), i16),
            pltpu.VMEM((2, 2, 2, 2, double, FEAT), i16),
            pltpu.VMEM((2, 2, 2, double, FEAT), i16),
            pltpu.VMEM((2, 2, 2, 2, double, FEAT), i16),
            pltpu.VMEM((2, 3, double, FEAT), i16),
            pltpu.VMEM((2, 3, double, FEAT), i16),
            pltpu.VMEM((2, HALF, FEAT), bf16),
            pltpu.VMEM((ROWS, FEAT), bf16),
            dma, dma, dma, dma,
            dma, dma((2,)), dma, dma((2,)), dma, dma((3,)),
            dma, dma((2, 16)), dma, dma((2, 8)), dma, dma((2,)),
            dma, dma((2, 2, 2)), dma, dma((2, 2)), dma, dma((2,)),
            dma, dma,
        ],
        compiler_params=pltpu.CompilerParams(collective_id=0, has_side_effects=True, vmem_limit_bytes=52 * 1024 * 1024),
    )(
        tokens,
        norm_gain,
        route_logits.T,
        expert_ids.T,
        active.reshape(1, FEAT),
        gate_weight.reshape(HID, WIDTH),
        up_weight.reshape(HID, WIDTH),
        down_weight.reshape(HID, WIDTH),
    )


def solution(mesh):
    split = Mesh(mesh.devices.reshape(ZS, SIDE, SIDE, 2), ("expert", "x", "y", "c"))
    plane = ("x", "y", "c")
    weight = P("expert", plane, None)
    in_specs = (P("expert", plane), P(), P("expert", None), P("expert", None), P("expert"), weight, weight, weight)
    return jax.shard_map(local, mesh=split, in_specs=in_specs, out_specs=P("expert", plane), check_vma=False)
```

```python
import jax
import jax.numpy as jnp
from jax import lax
from jax.experimental import pallas as pl
from jax.experimental.pallas import tpu as pltpu
from jax.sharding import Mesh
from jax.sharding import PartitionSpec as P

MESH = pl.DeviceIdType.MESH
EPS = 1e-05
ZS = 8
SIDE = 4
SEATS = 64
ROWS = ZS * SEATS
HALF = ROWS // 2
QUARTER = HALF // 2
FEAT = 128
HID = 448
WIDTH = 4096
QMAX = 32000.0

ORDER = [(0, 0), (3, 0), (1, 0), (0, 3), (0, 1), (2, 0), (3, 3), (3, 1), (1, 3), (1, 1), (0, 2), (2, 3), (2, 1), (3, 2), (1, 2), (2, 2)]
MIRROR = [ORDER.index((j, i)) for i, j in ORDER]
PRODUCTS = ((1, 3), (2, 4), (5, 10), (0, 6), (7, 8), (9, 11), (13, 12), (14, 15))
BLOCKS = ((2, 3), (1, 0))

SCHEDULE = (
    ("arr", 0, 1), ("arr", 0, 2), ("arr", 0, 3), ("arr", 1, 4), ("arr", 1, 3), ("arr", 0, 4),
    ("arr", 1, 1), ("scale", 0), ("arr", 0, 5), ("arr", 1, 2), ("scale", 1), ("weights",),
    ("prod", 1, 1), ("arr", 0, 6), ("arr", 0, 8), ("arr", 0, 7), ("prod", 1, 0), ("arr", 0, 9),
    ("arr", 0, 10), ("prod", 0, 1), ("arr", 1, 5), ("arr", 1, 10), ("arr", 1, 7), ("prod", 0, 3),
    ("prod", 0, 2), ("arr", 1, 6), ("arr", 0, 12), ("arr", 0, 11), ("prod", 0, 4), ("arr", 1, 8),
    ("arr", 1, 9), ("arr", 0, 13), ("arr", 0, 14), ("arr", 0, 15), ("prod", 0, 0), ("prod", 0, 5),
    ("prod", 0, 6), ("prod", 0, 7), ("hidden", 0), ("arr", 1, 13), ("arr", 1, 15), ("arr", 1, 11),
    ("down",), ("pre2", 0), ("arr", 1, 12), ("prod", 1, 3), ("prod", 1, 2), ("arr", 1, 14),
    ("p2", 0), ("ahead", 0, 0), ("ahead", 0, 1), ("pd", 0, 1), ("prod", 1, 6), ("direct", 0, 0, 1),
    ("prod", 1, 7), ("pd", 0, 0), ("direct", 0, 1, 0), ("direct", 0, 1, 1), ("prod", 1, 4), ("direct", 0, 0, 0),
    ("prod", 1, 5), ("hidden", 1), ("pre2", 1), ("joined", 0, 0, 0), ("joined", 0, 0, 1), ("joined", 0, 1, 0),
    ("joined", 0, 1, 1), ("p2", 1), ("ahead", 1, 0), ("ahead", 1, 1), ("p0", 0), ("pd", 1, 0),
    ("pd", 1, 1), ("direct", 1, 0, 0), ("direct", 1, 0, 1), ("direct", 1, 1, 1), ("direct", 1, 1, 0), ("sum", 0, 0),
    ("sum", 0, 2), ("sum", 0, 1), ("joined", 1, 0, 0), ("p0", 1), ("joined", 1, 0, 1), ("own", 0),
    ("joined", 1, 1, 0), ("joined", 1, 1, 1), ("finish", 0), ("sum", 1, 0), ("sum", 1, 2), ("own", 1),
    ("sum", 1, 1), ("finish", 1),
)


def encode(values, ref):
    row = lax.broadcasted_iota(jnp.int32, (16, FEAT), 0)
    scale = jnp.zeros((16, FEAT), jnp.int32)
    for n, v in enumerate(values):
        top = jnp.maximum(jnp.max(jnp.abs(v), axis=0, keepdims=True), 1e-30)
        exponent = jnp.ceil(jnp.log2(top))
        power = jnp.exp2(exponent)
        mantissa = jnp.ceil(top / power * QMAX)
        inverse = (QMAX * QMAX) / (mantissa * power)
        ref[n * QUARTER : (n + 1) * QUARTER, :] = jnp.round(v * inverse).astype(jnp.int32).astype(jnp.int16)
        scale = jnp.where(row >= 8 * n, jnp.where(row < 8 * n + 4, exponent.astype(jnp.int32), mantissa.astype(jnp.int32)), scale)
    ref[len(values) * QUARTER :, :] = scale.astype(jnp.int16)


def decode(ref, n=0):
    scale = ref[ref.shape[0] - 16 :, :].astype(jnp.int32).astype(jnp.float32)
    factor = scale[8 * n + 4 : 8 * n + 5, :] * jnp.exp2(scale[8 * n : 8 * n + 1, :]) * (1.0 / (QMAX * QMAX))
    return ref[n * QUARTER : (n + 1) * QUARTER, :].astype(jnp.int32).astype(jnp.float32) * factor


def column(row):
    return jnp.broadcast_to(row, (FEAT, FEAT)).T


def dot(a, b, dims, precision=None):
    return lax.dot_general(a, b, (dims, ((), ())), precision=precision, preferred_element_type=jnp.float32)


def kernel(
    tok_ref, gain_ref, logit_ref, ids_ref, act_ref, wg_hbm, wu_hbm, wd_hbm, out_ref,
    wide_w, dn, outbox, gathered, scale_rows, rsend, rrecv, turned, msb, xn, sums, hid, part, red,
    sfb, sdb, rfb, rdb, sda, rda, fin, ret,
    w_sem, dn_sem, dns_sem, dnr_sem, z_s, z_r, rz_s, rz_r, ms_s, ms_r, g_s, g_r, d_s, d_r, h_s, h_r,
    bf_s, bf_r, bd_s, bd_r, ad_s, ad_r, t_s, t_r,
):
    z, x, y, c = (lax.axis_index(n) for n in ("expert", "x", "y", "c"))
    a = jnp.where(c == 0, x, y)
    b = jnp.where(c == 0, y, x)
    mate = {"c": 1 - c}

    def wrap(v):
        return lax.rem(v, SIDE)

    def to_a(s):
        return {"x": wrap(x + s * (1 - c)), "y": wrap(y + s * c)}

    def to_b(s):
        return {"x": wrap(x + s * c), "y": wrap(y + s * (1 - c))}

    def to_z(s):
        return {"expert": lax.rem(z + s, ZS)}

    def remote(src, dst, s_sem, r_sem, device):
        pltpu.make_async_remote_copy(src_ref=src, dst_ref=dst, send_sem=s_sem, recv_sem=r_sem, device_id=device, device_id_type=MESH).start()

    def arrived(ref, sem):
        pltpu.make_async_copy(ref, ref, sem).wait()

    for n, w in enumerate((wg_hbm, wu_hbm)):
        pltpu.make_async_copy(w, wide_w.at[n], w_sem).start()

    def down_columns(aa, bb, core):
        xx = jnp.where(core == 0, aa, bb)
        yy = jnp.where(core == 0, bb, aa)
        return pl.ds(pl.multiple_of(((xx * SIDE + yy) * 2 + core) * FEAT, FEAT), FEAT)

    barrier = pltpu.get_barrier_semaphore()
    peers = [mate] + [{"x": wrap(x + s)} for s in (1, 2, 3)] + [{"y": wrap(y + s)} for s in (1, 2, 3)] + [to_z(s) for s in range(1, ZS)]
    for peer in peers:
        pl.semaphore_signal(barrier, inc=1, device_id=peer, device_id_type=MESH)

    for aa in range(SIDE):
        for bb in range(SIDE):
            pltpu.make_async_copy(wd_hbm.at[:, down_columns(aa, bb, c)], dn.at[c, bb, :, pl.ds(aa * FEAT, FEAT)], dn_sem).start()

    tok = tok_ref[...]
    wide = tok.astype(jnp.float32)
    msb[0] = jnp.sum((wide * wide).T, axis=0, keepdims=True)

    seat_row = lax.broadcasted_iota(jnp.int32, (ROWS, FEAT), 0)
    expert_of = seat_row // SEATS
    seat_of = (seat_row - expert_of * SEATS).astype(jnp.float32)
    live = jnp.broadcast_to(act_ref[...], (ROWS, FEAT)) > 0
    first = (expert_of == jnp.broadcast_to(ids_ref[0:1, :], (ROWS, FEAT))) & live
    second = (expert_of == jnp.broadcast_to(ids_ref[1:2, :], (ROWS, FEAT))) & live
    named = jnp.where(first | second, 1.0, 0.0)
    before = jnp.where(lax.broadcasted_iota(jnp.int32, (FEAT, FEAT), 0) < lax.broadcasted_iota(jnp.int32, (FEAT, FEAT), 1), 1.0, 0.0)
    position = dot(named.astype(jnp.bfloat16), before.astype(jnp.bfloat16), ((1,), (0,)))
    seated = position == seat_of
    pick0 = jnp.where(first & seated, 1.0, 0.0)
    pick1 = jnp.where(second & seated, 1.0, 0.0)
    pick = (pick0 + pick1).astype(jnp.bfloat16)
    outbox[...] = dot(pick, tok, ((1,), (0,))).astype(jnp.bfloat16)

    pl.semaphore_wait(barrier, len(peers))
    remote(msb.at[0], msb.at[1], ms_s, ms_r.at[0], mate)
    me = a * SIDE + b
    my_half = z // 4
    own_seats = pl.ds(pl.multiple_of(z * SEATS, SEATS), SEATS)
    landing = gathered.at[my_half, c, me, pl.ds(pl.multiple_of(z % 4 * SEATS, SEATS), SEATS)]
    for s in (4, 5, 3, 6, 2, 7, 1):
        target = lax.rem(z + s, ZS)
        remote(outbox.at[pl.ds(pl.multiple_of(target * SEATS, SEATS), SEATS)], landing, z_s, z_r.at[my_half], to_z(s))
    pltpu.make_async_copy(outbox.at[own_seats], landing, z_r.at[my_half]).start()
    for aa in range(SIDE):
        for bb in range(SIDE):
            remote(wd_hbm.at[:, down_columns(aa, bb, 1 - c)], dn.at[c, bb, :, pl.ds(aa * FEAT, FEAT)], dns_sem, dnr_sem, mate)

    def pass_on(h, i, j, quarter, device, di, dj):
        k = wrap(a + i) * SIDE + wrap(b + j)
        ref = gathered.at[h, c, k]
        if quarter is not None:
            ref = ref.at[pl.ds(quarter * QUARTER, QUARTER)]
        remote(ref, ref, g_s, g_r.at[h, ORDER.index(((i - di) % 4, (j - dj) % 4))], device)

    def arrive(h, n):
        i, j = ORDER[n]
        k = wrap(a + i) * SIDE + wrap(b + j)
        if n == 0:
            arrived(gathered.at[h, c, k], z_r.at[h])
            pass_on(h, 0, 0, None, to_a(1), 1, 0)
            pass_on(h, 0, 0, None, to_a(3), 3, 0)
            pass_on(h, 0, 0, None, to_a(2), 2, 0)
        else:
            arrived(gathered.at[h, c, k], g_r.at[h, n])
        if j == 0:
            pass_on(h, i, j, None, to_b(1), 0, 1)
            pass_on(h, i, j, None, to_b(3), 0, 3)
        if (i, j) == (2, 0):
            pass_on(h, i, j, None, to_b(2), 0, 2)
        if j == 3 and i != 2:
            pass_on(h, i, j, 0, to_b(1), 0, 1)
        if j == 1 and i != 2:
            pass_on(h, i, j, 1, to_b(3), 0, 3)
        group = next(g for g, pair in enumerate(PRODUCTS) if MIRROR[n] in pair)
        remote(gathered.at[h, c, k], gathered.at[h, c, k], d_s, d_r.at[h, group], mate)

    opened = set()

    def product(h, group):
        arrived(gathered.at[h, 0, pl.ds(0, 2)], d_r.at[h, group])
        offsets = []
        for p, n in enumerate(PRODUCTS[group]):
            i, j = ORDER[n]
            aa, bb = wrap(a + i), wrap(b + j)
            mine, other = aa * SIDE + bb, bb * SIDE + aa
            chip = jnp.where(c == 0, mine, other)
            at = pl.ds(pl.multiple_of(chip * 2 * FEAT, 2 * FEAT), 2 * FEAT)
            gains = gain_ref[at].astype(jnp.float32).reshape(1, 2 * FEAT)
            for core in (0, 1):
                k = jnp.where(c == core, mine, other)
                lanes = slice(core * FEAT, (core + 1) * FEAT)
                normed = gathered[h, core, k].astype(jnp.float32) * scale_rows[h] * gains[:, lanes]
                xn[p, :, lanes] = normed.astype(jnp.bfloat16)
            offsets.append(at)
        for n in (0, 1):
            terms = sum(dot(wide_w[n, :, at], xn[p], ((1,), (1,))) for p, at in enumerate(offsets))
            sums[h, n] = sums[h, n] + terms if h in opened else terms
        opened.add(h)

    def hidden(h):
        g = sums[h, 0]
        hid[h, c] = (g / (1.0 + jnp.exp(-g)) * sums[h, 1]).T.astype(jnp.bfloat16)
        remote(hid.at[h, c], hid.at[h, c], h_s, h_r.at[h], mate)

    AHEAD, STEP, SIDES = 2, (1, 3), (1, 3)

    def partial(h, j, own, first):
        core = c if own else 1 - c
        terms = dot(hid[h, core], dn[core, wrap(b + j)], ((1,), (0,)))
        part[h, j] = terms if first else part[h, j] + terms

    def block(h, j, q, i):
        return part[h, j, q * QUARTER : (q + 1) * QUARTER, pl.ds(pl.multiple_of(wrap(a + i) * FEAT, FEAT), FEAT)]

    def send_ahead(h, g):
        for d in (0, 1):
            encode([block(h, AHEAD, d, i) for i in BLOCKS[g]], sfb.at[h, d, g])
            remote(sfb.at[h, d, g], rfb.at[h, d, g], bf_s, bf_r.at[h, d, g], to_b(STEP[d]))

    def send_direct(h, g, d):
        q = 1 - d
        encode([block(h, SIDES[d], q, i) for i in BLOCKS[g]], sdb.at[h, g, d, q])
        remote(sdb.at[h, g, d, q], rdb.at[h, g, d, q], bd_s, bd_r.at[h, g], to_b(STEP[d]))

    def send_joined(h, g, d):
        q = d
        arrived(rfb.at[h, d, g], bf_r.at[h, d, g])
        encode([block(h, SIDES[d], q, i) + decode(rfb.at[h, d, g], n) for n, i in enumerate(BLOCKS[g])], sdb.at[h, g, d, q])
        remote(sdb.at[h, g, d, q], rdb.at[h, g, d, q], bd_s, bd_r.at[h, g], to_b(STEP[d]))

    awaited = set()

    def summed(h, i):
        g = 0 if i in BLOCKS[0] else 1
        n = BLOCKS[g].index(i)
        if (h, g) not in awaited:
            awaited.add((h, g))
            arrived(rdb.at[h, g], bd_r.at[h, g])
        return [block(h, 0, q, i) + decode(rdb.at[h, g, 0, q], n) + decode(rdb.at[h, g, 1, q], n) for q in (0, 1)]

    def send_sum(h, n):
        i = (2, 1, 3)[n]
        encode(summed(h, i), sda.at[h, n])
        remote(sda.at[h, n], rda.at[h, n], ad_s, ad_r.at[h], to_a(i))

    def keep_sum(h):
        red[h, 0], red[h, 1] = summed(h, 0)

    def finish(h):
        arrived(rda.at[h], ad_r.at[h])
        for q in (0, 1):
            total = red[h, q] + decode(rda.at[h, 0], q) + decode(rda.at[h, 1], q) + decode(rda.at[h, 2], q)
            fin[h, q * QUARTER : (q + 1) * QUARTER, :] = total.astype(jnp.bfloat16)
        for m in range(4):
            g = h * 4 + m
            source, target = fin.at[h, pl.ds(m * SEATS, SEATS)], ret.at[own_seats]

            @pl.when(z != g)
            def _():
                remote(source, target, t_s, t_r, {"expert": g})

            @pl.when(z == g)
            def _():
                pltpu.make_async_copy(source, target, t_r).start()

    arrived(msb.at[1], ms_r.at[0])
    msb[2] = msb[0] + msb[1]
    for s in (1, 2, 3):
        remote(msb.at[2], msb.at[2 + s], ms_s, ms_r.at[1], {"x": wrap(x + s)})
    arrived(msb.at[pl.ds(3, 3)], ms_r.at[1])
    msb[6] = (msb[2] + msb[3]) + (msb[4] + msb[5])
    for s in (1, 2, 3):
        remote(msb.at[6], msb.at[6 + s], ms_s, ms_r.at[2], {"y": wrap(y + s)})
    arrive(0, 0)
    arrive(1, 0)
    arrived(msb.at[pl.ds(7, 3)], ms_r.at[2])
    mean_square = ((msb[6] + msb[7]) + (msb[8] + msb[9])) / WIDTH
    inverse = lax.rsqrt(mean_square + EPS)
    rsend[...] = dot(jnp.broadcast_to(inverse, (8, FEAT)), pick.astype(jnp.float32), ((1,), (1,)), lax.Precision.HIGHEST)[0:1, :]
    for s in range(1, ZS):
        remote(rsend, rrecv.at[z], rz_s, rz_r.at[my_half], to_z(s))
    pltpu.make_async_copy(rsend, rrecv.at[z], rz_r.at[my_half]).start()
    l0, l1 = logit_ref[0:1, :], logit_ref[1:2, :]
    high = jnp.maximum(l0, l1)
    e0, e1 = jnp.exp(l0 - high), jnp.exp(l1 - high)
    alive = act_ref[...].astype(jnp.float32)
    prob0 = column(e0 / (e0 + e1) * alive)
    prob1 = column(e1 / (e0 + e1) * alive)

    lane_block = pl.ds(pl.multiple_of(z // 2 * FEAT, FEAT), FEAT)
    seat_block = pl.ds(pl.multiple_of(z % 2 * SEATS, SEATS), SEATS)

    def scales(h):
        arrived(rrecv.at[pl.ds(0, 4)], rz_r.at[h])
        for m in range(4):
            turned[...] = column(rrecv[h * 4 + m, :, lane_block])
            scale_rows[h, m * SEATS : (m + 1) * SEATS, :] = turned[seat_block, :]

    def down_ready():
        arrived(dn.at[c], dn_sem)
        arrived(dn.at[1 - c], dnr_sem)

    def weights_ready():
        arrived(wide_w, w_sem)

    def both_cores(h):
        arrived(hid.at[h, 1 - c], h_r.at[h])
        partial(h, AHEAD, False, False)

    def whole_partial(h, j):
        partial(h, j, True, True)
        partial(h, j, False, False)

    events = {
        "arr": arrive,
        "scale": scales,
        "weights": weights_ready,
        "prod": product,
        "hidden": hidden,
        "down": down_ready,
        "pre2": lambda h: partial(h, AHEAD, True, True),
        "p2": both_cores,
        "ahead": send_ahead,
        "pd": lambda h, d: whole_partial(h, SIDES[d]),
        "direct": send_direct,
        "joined": send_joined,
        "p0": lambda h: whole_partial(h, 0),
        "sum": send_sum,
        "own": keep_sum,
        "finish": finish,
    }
    for name, *which in SCHEDULE:
        events[name](*which)
    arrived(ret, t_r)
    back = ret[...]
    from0 = dot(pick0.astype(jnp.bfloat16), back, ((0,), (0,)))
    from1 = dot(pick1.astype(jnp.bfloat16), back, ((0,), (0,)))
    out_ref[...] = (prob0 * from0 + prob1 * from1).astype(jnp.bfloat16)

    arrived(outbox.at[pl.ds(0, ROWS - SEATS)], z_s)
    arrived(rrecv.at[pl.ds(0, ZS - 1)], rz_s)
    arrived(msb.at[pl.ds(0, 7)], ms_s)
    arrived(gathered.at[:, 0, pl.ds(0, 15)], g_s)
    arrived(gathered.at[:, 0], d_s)
    arrived(hid.at[:, 0], h_s)
    arrived(sfb, bf_s)
    arrived(sdb, bd_s)
    arrived(sda, ad_s)
    arrived(ret.at[pl.ds(0, ROWS - SEATS)], t_s)
    arrived(dn.at[c], dns_sem)


def local(tokens, norm_gain, route_logits, expert_ids, active, gate_weight, up_weight, down_weight):
    vmem = pl.BlockSpec(memory_space=pltpu.VMEM)
    hbm = pl.BlockSpec(memory_space=pltpu.HBM)
    bf16, f32, i16 = jnp.bfloat16, jnp.float32, jnp.int16
    dma = pltpu.SemaphoreType.DMA
    double = 2 * QUARTER + 16
    return pl.pallas_call(
        kernel,
        out_shape=jax.ShapeDtypeStruct((FEAT, FEAT), bf16),
        in_specs=[vmem] * 5 + [hbm] * 3,
        out_specs=vmem,
        scratch_shapes=[
            pltpu.VMEM((2, HID, WIDTH), bf16),
            pltpu.VMEM((2, SIDE, HID, SIDE * FEAT), bf16),
            pltpu.VMEM((ROWS, FEAT), bf16),
            pltpu.VMEM((2, 2, 16, HALF, FEAT), bf16),
            pltpu.VMEM((2, HALF, FEAT), f32),
            pltpu.VMEM((1, ROWS), f32),
            pltpu.VMEM((ZS, 1, ROWS), f32),
            pltpu.VMEM((FEAT, FEAT), f32),
            pltpu.VMEM((10, 1, FEAT), f32),
            pltpu.VMEM((2, HALF, 2 * FEAT), bf16),
            pltpu.VMEM((2, 2, HID, HALF), f32),
            pltpu.VMEM((2, 2, HALF, HID), bf16),
            pltpu.VMEM((2, SIDE, HALF, SIDE * FEAT), f32),
            pltpu.VMEM((2, 2, QUARTER, FEAT), f32),
            pltpu.VMEM((2, 2, 2, double, FEAT), i16),
            pltpu.VMEM((2, 2, 2, 2, double, FEAT), i16),
            pltpu.VMEM((2, 2, 2, double, FEAT), i16),
            pltpu.VMEM((2, 2, 2, 2, double, FEAT), i16),
            pltpu.VMEM((2, 3, double, FEAT), i16),
            pltpu.VMEM((2, 3, double, FEAT), i16),
            pltpu.VMEM((2, HALF, FEAT), bf16),
            pltpu.VMEM((ROWS, FEAT), bf16),
            dma, dma, dma, dma,
            dma, dma((2,)), dma, dma((2,)), dma, dma((3,)),
            dma, dma((2, 16)), dma, dma((2, 8)), dma, dma((2,)),
            dma, dma((2, 2, 2)), dma, dma((2, 2)), dma, dma((2,)),
            dma, dma,
        ],
        compiler_params=pltpu.CompilerParams(collective_id=0, has_side_effects=True, vmem_limit_bytes=52 * 1024 * 1024),
    )(
        tokens,
        norm_gain,
        route_logits.T,
        expert_ids.T,
        active.reshape(1, FEAT),
        gate_weight.reshape(HID, WIDTH),
        up_weight.reshape(HID, WIDTH),
        down_weight.reshape(HID, WIDTH),
    )


def solution(mesh):
    split = Mesh(mesh.devices.reshape(ZS, SIDE, SIDE, 2), ("expert", "x", "y", "c"))
    plane = ("x", "y", "c")
    weight = P("expert", plane, None)
    in_specs = (P("expert", plane), P(), P("expert", None), P("expert", None), P("expert"), weight, weight, weight)
    return jax.shard_map(local, mesh=split, in_specs=in_specs, out_specs=P("expert", plane), check_vma=False)
```

```python
import jax
import jax.numpy as jnp
from jax import lax
from jax.experimental import pallas as pl
from jax.experimental.pallas import tpu as pltpu
from jax.sharding import Mesh
from jax.sharding import PartitionSpec as P

MESH = pl.DeviceIdType.MESH
EPS = 1e-05
ZS = 8
SIDE = 4
SEATS = 64
ROWS = ZS * SEATS
HALF = ROWS // 2
QUARTER = HALF // 2
FEAT = 128
HID = 448
WIDTH = 4096
QMAX = 32000.0

ORDER = [(0, 0), (3, 0), (1, 0), (0, 3), (0, 1), (2, 0), (3, 3), (3, 1), (1, 3), (1, 1), (0, 2), (2, 3), (2, 1), (3, 2), (1, 2), (2, 2)]
MIRROR = [ORDER.index((j, i)) for i, j in ORDER]
PRODUCTS = ((1, 3), (2, 4), (5, 10), (0, 6), (7, 8), (9, 11), (13, 12), (14, 15))
BLOCKS = ((2, 3), (1, 0))

SCHEDULE = (
    ("arr", 0, 1), ("arr", 0, 2), ("arr", 0, 4), ("arr", 0, 3), ("arr", 0, 5), ("scale", 0),
    ("arr", 1, 1), ("arr", 0, 7), ("arr", 0, 6), ("arr", 0, 9), ("arr", 0, 8), ("weights",),
    ("prod", 0, 1), ("arr", 0, 10), ("arr", 1, 4), ("arr", 1, 2), ("prod", 0, 3), ("arr", 1, 5),
    ("prod", 0, 2), ("arr", 1, 3), ("prod", 0, 0), ("arr", 0, 12), ("scale", 1), ("arr", 0, 15),
    ("arr", 1, 7), ("arr", 0, 11), ("arr", 0, 13), ("prod", 0, 4), ("arr", 0, 14), ("arr", 1, 6),
    ("prod", 1, 0), ("prod", 0, 7), ("prod", 0, 5), ("prod", 0, 6), ("hidden", 0), ("arr", 1, 9),
    ("down",), ("pre2", 0), ("arr", 1, 11), ("arr", 1, 12), ("arr", 1, 8), ("prod", 1, 1),
    ("arr", 1, 10), ("prod", 1, 3), ("p2", 0), ("ahead", 0, 0), ("ahead", 0, 1), ("pd", 0, 0),
    ("arr", 1, 15), ("prod", 1, 4), ("prod", 1, 2), ("arr", 1, 13), ("pd", 0, 1), ("arr", 1, 14),
    ("direct", 0, 1, 1), ("direct", 0, 1, 0), ("prod", 1, 7), ("direct", 0, 0, 1), ("prod", 1, 5), ("direct", 0, 0, 0),
    ("prod", 1, 6), ("hidden", 1), ("joined", 0, 0, 1), ("joined", 0, 0, 0), ("joined", 0, 1, 1), ("joined", 0, 1, 0),
    ("pre2", 1), ("p2", 1), ("ahead", 1, 0), ("ahead", 1, 1), ("pd", 1, 1), ("pd", 1, 0),
    ("direct", 1, 1, 0), ("direct", 1, 0, 1), ("direct", 1, 0, 0), ("p0", 0), ("direct", 1, 1, 1), ("p0", 1),
    ("sum", 0, 0), ("sum", 0, 1), ("sum", 0, 2), ("joined", 1, 0, 1), ("own", 0), ("joined", 1, 0, 0),
    ("joined", 1, 1, 1), ("joined", 1, 1, 0), ("finish", 0), ("sum", 1, 0), ("sum", 1, 2), ("sum", 1, 1),
    ("own", 1), ("finish", 1),
)


def encode(values, ref):
    row = lax.broadcasted_iota(jnp.int32, (16, FEAT), 0)
    scale = jnp.zeros((16, FEAT), jnp.int32)
    for n, v in enumerate(values):
        top = jnp.maximum(jnp.max(jnp.abs(v), axis=0, keepdims=True), 1e-30)
        exponent = jnp.ceil(jnp.log2(top))
        power = jnp.exp2(exponent)
        mantissa = jnp.ceil(top / power * QMAX)
        inverse = (QMAX * QMAX) / (mantissa * power)
        ref[n * QUARTER : (n + 1) * QUARTER, :] = jnp.round(v * inverse).astype(jnp.int32).astype(jnp.int16)
        scale = jnp.where(row >= 8 * n, jnp.where(row < 8 * n + 4, exponent.astype(jnp.int32), mantissa.astype(jnp.int32)), scale)
    ref[len(values) * QUARTER :, :] = scale.astype(jnp.int16)


def decode(ref, n=0):
    scale = ref[ref.shape[0] - 16 :, :].astype(jnp.int32).astype(jnp.float32)
    factor = scale[8 * n + 4 : 8 * n + 5, :] * jnp.exp2(scale[8 * n : 8 * n + 1, :]) * (1.0 / (QMAX * QMAX))
    return ref[n * QUARTER : (n + 1) * QUARTER, :].astype(jnp.int32).astype(jnp.float32) * factor


def column(row):
    return jnp.broadcast_to(row, (FEAT, FEAT)).T


def dot(a, b, dims, precision=None):
    return lax.dot_general(a, b, (dims, ((), ())), precision=precision, preferred_element_type=jnp.float32)


def kernel(
    tok_hbm, gain_hbm, logit_hbm, ids_hbm, act_hbm, wg_hbm, wu_hbm, wd_hbm, out_ref,
    tok_ref, gain_ref, logit_ref, ids_ref, act_ref,
    wide_w, dn, outbox, gathered, scale_rows, rsend, rrecv, turned, msb, xn, sums, hid, part, red,
    sfb, sdb, rfb, rdb, sda, rda, fin, ret,
    in_sem, w_sem, dn_sem, dns_sem, dnr_sem, z_s, z_r, rz_s, rz_r, ms_s, ms_r, g_s, g_r, d_s, d_r, h_s, h_r,
    bf_s, bf_r, bd_s, bd_r, ad_s, ad_r, t_s, t_r,
):
    z, x, y, c = (lax.axis_index(n) for n in ("expert", "x", "y", "c"))
    a = jnp.where(c == 0, x, y)
    b = jnp.where(c == 0, y, x)
    mate = {"c": 1 - c}

    def wrap(v):
        return lax.rem(v, SIDE)

    def to_a(s):
        return {"x": wrap(x + s * (1 - c)), "y": wrap(y + s * c)}

    def to_b(s):
        return {"x": wrap(x + s * c), "y": wrap(y + s * (1 - c))}

    def to_z(s):
        return {"expert": lax.rem(z + s, ZS)}

    def remote(src, dst, s_sem, r_sem, device):
        pltpu.make_async_remote_copy(src_ref=src, dst_ref=dst, send_sem=s_sem, recv_sem=r_sem, device_id=device, device_id_type=MESH).start()

    def arrived(ref, sem):
        pltpu.make_async_copy(ref, ref, sem).wait()

    def down_columns(aa, bb, core):
        xx = jnp.where(core == 0, aa, bb)
        yy = jnp.where(core == 0, bb, aa)
        return pl.ds(pl.multiple_of(((xx * SIDE + yy) * 2 + core) * FEAT, FEAT), FEAT)

    small = ((tok_hbm, tok_ref), (act_hbm, act_ref), (ids_hbm, ids_ref), (logit_hbm, logit_ref), (gain_hbm, gain_ref))
    small = [pltpu.make_async_copy(source, target, in_sem.at[n]) for n, (source, target) in enumerate(small)]
    for copy in small:
        copy.start()
    barrier = pltpu.get_barrier_semaphore()
    peers = [mate] + [{"x": wrap(x + s)} for s in (1, 2, 3)] + [{"y": wrap(y + s)} for s in (1, 2, 3)] + [to_z(s) for s in range(1, ZS)]
    for peer in peers:
        pl.semaphore_signal(barrier, inc=1, device_id=peer, device_id_type=MESH)

    for copy in small[:3]:
        copy.wait()
    for n, w in enumerate((wg_hbm, wu_hbm)):
        pltpu.make_async_copy(w, wide_w.at[n], w_sem).start()
    for aa in range(SIDE):
        for bb in range(SIDE):
            pltpu.make_async_copy(wd_hbm.at[:, down_columns(aa, bb, c)], dn.at[c, bb, :, pl.ds(aa * FEAT, FEAT)], dn_sem).start()

    tok = tok_ref[...]
    wide = tok.astype(jnp.float32)
    msb[0] = jnp.sum((wide * wide).T, axis=0, keepdims=True)

    seat_row = lax.broadcasted_iota(jnp.int32, (ROWS, FEAT), 0)
    expert_of = seat_row // SEATS
    seat_of = (seat_row - expert_of * SEATS).astype(jnp.float32)
    live = jnp.broadcast_to(act_ref[...], (ROWS, FEAT)) > 0
    first = (expert_of == jnp.broadcast_to(ids_ref[0:1, :], (ROWS, FEAT))) & live
    second = (expert_of == jnp.broadcast_to(ids_ref[1:2, :], (ROWS, FEAT))) & live
    named = jnp.where(first | second, 1.0, 0.0)
    before = jnp.where(lax.broadcasted_iota(jnp.int32, (FEAT, FEAT), 0) < lax.broadcasted_iota(jnp.int32, (FEAT, FEAT), 1), 1.0, 0.0)
    position = dot(named.astype(jnp.bfloat16), before.astype(jnp.bfloat16), ((1,), (0,)))
    seated = position == seat_of
    pick0 = jnp.where(first & seated, 1.0, 0.0)
    pick1 = jnp.where(second & seated, 1.0, 0.0)
    pick = (pick0 + pick1).astype(jnp.bfloat16)
    outbox[...] = dot(pick, tok, ((1,), (0,))).astype(jnp.bfloat16)

    pl.semaphore_wait(barrier, len(peers))
    remote(msb.at[0], msb.at[1], ms_s, ms_r.at[0], mate)
    me = a * SIDE + b
    my_half = z // 4
    own_seats = pl.ds(pl.multiple_of(z * SEATS, SEATS), SEATS)
    landing = gathered.at[my_half, c, me, pl.ds(pl.multiple_of(z % 4 * SEATS, SEATS), SEATS)]
    for s in (4, 5, 3, 6, 2, 7, 1):
        target = lax.rem(z + s, ZS)
        remote(outbox.at[pl.ds(pl.multiple_of(target * SEATS, SEATS), SEATS)], landing, z_s, z_r.at[my_half], to_z(s))
    pltpu.make_async_copy(outbox.at[own_seats], landing, z_r.at[my_half]).start()
    for aa in range(SIDE):
        for bb in range(SIDE):
            remote(wd_hbm.at[:, down_columns(aa, bb, 1 - c)], dn.at[c, bb, :, pl.ds(aa * FEAT, FEAT)], dns_sem, dnr_sem, mate)

    def pass_on(h, i, j, quarter, device, di, dj):
        k = wrap(a + i) * SIDE + wrap(b + j)
        ref = gathered.at[h, c, k]
        if quarter is not None:
            ref = ref.at[pl.ds(quarter * QUARTER, QUARTER)]
        remote(ref, ref, g_s, g_r.at[h, ORDER.index(((i - di) % 4, (j - dj) % 4))], device)

    def arrive(h, n):
        i, j = ORDER[n]
        k = wrap(a + i) * SIDE + wrap(b + j)
        if n == 0:
            arrived(gathered.at[h, c, k], z_r.at[h])
            pass_on(h, 0, 0, None, to_a(1), 1, 0)
            pass_on(h, 0, 0, None, to_a(3), 3, 0)
            pass_on(h, 0, 0, None, to_a(2), 2, 0)
        else:
            arrived(gathered.at[h, c, k], g_r.at[h, n])
        if j == 0:
            pass_on(h, i, j, None, to_b(1), 0, 1)
            pass_on(h, i, j, None, to_b(3), 0, 3)
        if (i, j) == (2, 0):
            pass_on(h, i, j, None, to_b(2), 0, 2)
        if j == 3 and i != 2:
            pass_on(h, i, j, 0, to_b(1), 0, 1)
        if j == 1 and i != 2:
            pass_on(h, i, j, 1, to_b(3), 0, 3)
        group = next(g for g, pair in enumerate(PRODUCTS) if MIRROR[n] in pair)
        remote(gathered.at[h, c, k], gathered.at[h, c, k], d_s, d_r.at[h, group], mate)

    opened = set()

    def product(h, group):
        arrived(gathered.at[h, 0, pl.ds(0, 2)], d_r.at[h, group])
        offsets = []
        for p, n in enumerate(PRODUCTS[group]):
            i, j = ORDER[n]
            aa, bb = wrap(a + i), wrap(b + j)
            mine, other = aa * SIDE + bb, bb * SIDE + aa
            chip = jnp.where(c == 0, mine, other)
            at = pl.ds(pl.multiple_of(chip * 2 * FEAT, 2 * FEAT), 2 * FEAT)
            gains = gain_ref[at].astype(jnp.float32).reshape(1, 2 * FEAT)
            for core in (0, 1):
                k = jnp.where(c == core, mine, other)
                lanes = slice(core * FEAT, (core + 1) * FEAT)
                normed = gathered[h, core, k].astype(jnp.float32) * scale_rows[h] * gains[:, lanes]
                xn[p, :, lanes] = normed.astype(jnp.bfloat16)
            offsets.append(at)
        for n in (0, 1):
            terms = sum(dot(wide_w[n, :, at], xn[p], ((1,), (1,))) for p, at in enumerate(offsets))
            sums[h, n] = sums[h, n] + terms if h in opened else terms
        opened.add(h)

    def hidden(h):
        g = sums[h, 0]
        hid[h, c] = (g / (1.0 + jnp.exp(-g)) * sums[h, 1]).T.astype(jnp.bfloat16)
        remote(hid.at[h, c], hid.at[h, c], h_s, h_r.at[h], mate)

    AHEAD, STEP, SIDES = 2, (1, 3), (1, 3)

    def partial(h, j, own, first):
        core = c if own else 1 - c
        terms = dot(hid[h, core], dn[core, wrap(b + j)], ((1,), (0,)))
        part[h, j] = terms if first else part[h, j] + terms

    def block(h, j, q, i):
        return part[h, j, q * QUARTER : (q + 1) * QUARTER, pl.ds(pl.multiple_of(wrap(a + i) * FEAT, FEAT), FEAT)]

    def send_ahead(h, g):
        for d in (0, 1):
            encode([block(h, AHEAD, d, i) for i in BLOCKS[g]], sfb.at[h, d, g])
            remote(sfb.at[h, d, g], rfb.at[h, d, g], bf_s, bf_r.at[h, d, g], to_b(STEP[d]))

    def send_direct(h, g, d):
        q = 1 - d
        encode([block(h, SIDES[d], q, i) for i in BLOCKS[g]], sdb.at[h, g, d, q])
        remote(sdb.at[h, g, d, q], rdb.at[h, g, d, q], bd_s, bd_r.at[h, g], to_b(STEP[d]))

    def send_joined(h, g, d):
        q = d
        arrived(rfb.at[h, d, g], bf_r.at[h, d, g])
        encode([block(h, SIDES[d], q, i) + decode(rfb.at[h, d, g], n) for n, i in enumerate(BLOCKS[g])], sdb.at[h, g, d, q])
        remote(sdb.at[h, g, d, q], rdb.at[h, g, d, q], bd_s, bd_r.at[h, g], to_b(STEP[d]))

    awaited = set()

    def summed(h, i):
        g = 0 if i in BLOCKS[0] else 1
        n = BLOCKS[g].index(i)
        if (h, g) not in awaited:
            awaited.add((h, g))
            arrived(rdb.at[h, g], bd_r.at[h, g])
        return [block(h, 0, q, i) + decode(rdb.at[h, g, 0, q], n) + decode(rdb.at[h, g, 1, q], n) for q in (0, 1)]

    def send_sum(h, n):
        i = (2, 1, 3)[n]
        encode(summed(h, i), sda.at[h, n])
        remote(sda.at[h, n], rda.at[h, n], ad_s, ad_r.at[h], to_a(i))

    def keep_sum(h):
        red[h, 0], red[h, 1] = summed(h, 0)

    def finish(h):
        arrived(rda.at[h], ad_r.at[h])
        for q in (0, 1):
            total = red[h, q] + decode(rda.at[h, 0], q) + decode(rda.at[h, 1], q) + decode(rda.at[h, 2], q)
            fin[h, q * QUARTER : (q + 1) * QUARTER, :] = total.astype(jnp.bfloat16)
        for m in range(4):
            g = h * 4 + m
            source, target = fin.at[h, pl.ds(m * SEATS, SEATS)], ret.at[own_seats]

            @pl.when(z != g)
            def _():
                remote(source, target, t_s, t_r, {"expert": g})

            @pl.when(z == g)
            def _():
                pltpu.make_async_copy(source, target, t_r).start()

    arrived(msb.at[1], ms_r.at[0])
    msb[2] = msb[0] + msb[1]
    for s in (1, 2, 3):
        remote(msb.at[2], msb.at[2 + s], ms_s, ms_r.at[1], {"x": wrap(x + s)})
    arrived(msb.at[pl.ds(3, 3)], ms_r.at[1])
    msb[6] = (msb[2] + msb[3]) + (msb[4] + msb[5])
    for s in (1, 2, 3):
        remote(msb.at[6], msb.at[6 + s], ms_s, ms_r.at[2], {"y": wrap(y + s)})
    arrive(0, 0)
    arrive(1, 0)
    arrived(msb.at[pl.ds(7, 3)], ms_r.at[2])
    mean_square = ((msb[6] + msb[7]) + (msb[8] + msb[9])) / WIDTH
    inverse = lax.rsqrt(mean_square + EPS)
    rsend[...] = dot(jnp.broadcast_to(inverse, (8, FEAT)), pick.astype(jnp.float32), ((1,), (1,)), lax.Precision.HIGHEST)[0:1, :]
    for s in range(1, ZS):
        remote(rsend, rrecv.at[z], rz_s, rz_r.at[my_half], to_z(s))
    pltpu.make_async_copy(rsend, rrecv.at[z], rz_r.at[my_half]).start()
    for copy in small[3:]:
        copy.wait()
    l0, l1 = logit_ref[0:1, :], logit_ref[1:2, :]
    high = jnp.maximum(l0, l1)
    e0, e1 = jnp.exp(l0 - high), jnp.exp(l1 - high)
    alive = act_ref[...].astype(jnp.float32)
    prob0 = column(e0 / (e0 + e1) * alive)
    prob1 = column(e1 / (e0 + e1) * alive)

    lane_block = pl.ds(pl.multiple_of(z // 2 * FEAT, FEAT), FEAT)
    seat_block = pl.ds(pl.multiple_of(z % 2 * SEATS, SEATS), SEATS)

    def scales(h):
        arrived(rrecv.at[pl.ds(0, 4)], rz_r.at[h])
        for m in range(4):
            turned[...] = column(rrecv[h * 4 + m, :, lane_block])
            scale_rows[h, m * SEATS : (m + 1) * SEATS, :] = turned[seat_block, :]

    def down_ready():
        arrived(dn.at[c], dn_sem)
        arrived(dn.at[1 - c], dnr_sem)

    def weights_ready():
        arrived(wide_w, w_sem)

    def both_cores(h):
        arrived(hid.at[h, 1 - c], h_r.at[h])
        partial(h, AHEAD, False, False)

    def whole_partial(h, j):
        partial(h, j, True, True)
        partial(h, j, False, False)

    events = {
        "arr": arrive,
        "scale": scales,
        "weights": weights_ready,
        "prod": product,
        "hidden": hidden,
        "down": down_ready,
        "pre2": lambda h: partial(h, AHEAD, True, True),
        "p2": both_cores,
        "ahead": send_ahead,
        "pd": lambda h, d: whole_partial(h, SIDES[d]),
        "direct": send_direct,
        "joined": send_joined,
        "p0": lambda h: whole_partial(h, 0),
        "sum": send_sum,
        "own": keep_sum,
        "finish": finish,
    }
    for name, *which in SCHEDULE:
        events[name](*which)
    arrived(ret, t_r)
    back = ret[...]
    from0 = dot(pick0.astype(jnp.bfloat16), back, ((0,), (0,)))
    from1 = dot(pick1.astype(jnp.bfloat16), back, ((0,), (0,)))
    out_ref[...] = (prob0 * from0 + prob1 * from1).astype(jnp.bfloat16)

    arrived(outbox.at[pl.ds(0, ROWS - SEATS)], z_s)
    arrived(rrecv.at[pl.ds(0, ZS - 1)], rz_s)
    arrived(msb.at[pl.ds(0, 7)], ms_s)
    arrived(gathered.at[:, 0, pl.ds(0, 15)], g_s)
    arrived(gathered.at[:, 0], d_s)
    arrived(hid.at[:, 0], h_s)
    arrived(sfb, bf_s)
    arrived(sdb, bd_s)
    arrived(sda, ad_s)
    arrived(ret.at[pl.ds(0, ROWS - SEATS)], t_s)
    arrived(dn.at[c], dns_sem)


def local(tokens, norm_gain, route_logits, expert_ids, active, gate_weight, up_weight, down_weight):
    vmem = pl.BlockSpec(memory_space=pltpu.VMEM)
    hbm = pl.BlockSpec(memory_space=pltpu.HBM)
    bf16, f32, i16 = jnp.bfloat16, jnp.float32, jnp.int16
    dma = pltpu.SemaphoreType.DMA
    double = 2 * QUARTER + 16

    def pin(v):
        return pltpu.with_memory_space_constraint(v, pltpu.HBM)

    return pl.pallas_call(
        kernel,
        out_shape=jax.ShapeDtypeStruct((FEAT, FEAT), bf16),
        in_specs=[hbm] * 8,
        out_specs=vmem,
        scratch_shapes=[
            pltpu.VMEM((FEAT, FEAT), bf16),
            pltpu.VMEM((WIDTH,), bf16),
            pltpu.VMEM((2, FEAT), f32),
            pltpu.VMEM((2, FEAT), jnp.int32),
            pltpu.VMEM((1, FEAT), jnp.int32),
            pltpu.VMEM((2, HID, WIDTH), bf16),
            pltpu.VMEM((2, SIDE, HID, SIDE * FEAT), bf16),
            pltpu.VMEM((ROWS, FEAT), bf16),
            pltpu.VMEM((2, 2, 16, HALF, FEAT), bf16),
            pltpu.VMEM((2, HALF, FEAT), f32),
            pltpu.VMEM((1, ROWS), f32),
            pltpu.VMEM((ZS, 1, ROWS), f32),
            pltpu.VMEM((FEAT, FEAT), f32),
            pltpu.VMEM((10, 1, FEAT), f32),
            pltpu.VMEM((2, HALF, 2 * FEAT), bf16),
            pltpu.VMEM((2, 2, HID, HALF), f32),
            pltpu.VMEM((2, 2, HALF, HID), bf16),
            pltpu.VMEM((2, SIDE, HALF, SIDE * FEAT), f32),
            pltpu.VMEM((2, 2, QUARTER, FEAT), f32),
            pltpu.VMEM((2, 2, 2, double, FEAT), i16),
            pltpu.VMEM((2, 2, 2, 2, double, FEAT), i16),
            pltpu.VMEM((2, 2, 2, double, FEAT), i16),
            pltpu.VMEM((2, 2, 2, 2, double, FEAT), i16),
            pltpu.VMEM((2, 3, double, FEAT), i16),
            pltpu.VMEM((2, 3, double, FEAT), i16),
            pltpu.VMEM((2, HALF, FEAT), bf16),
            pltpu.VMEM((ROWS, FEAT), bf16),
            dma((5,)), dma, dma, dma, dma,
            dma, dma((2,)), dma, dma((2,)), dma, dma((3,)),
            dma, dma((2, 16)), dma, dma((2, 8)), dma, dma((2,)),
            dma, dma((2, 2, 2)), dma, dma((2, 2)), dma, dma((2,)),
            dma, dma,
        ],
        compiler_params=pltpu.CompilerParams(collective_id=0, has_side_effects=True, vmem_limit_bytes=52 * 1024 * 1024),
    )(
        pin(tokens),
        pin(norm_gain),
        pin(route_logits.T),
        pin(expert_ids.T),
        pin(active.reshape(1, FEAT)),
        gate_weight.reshape(HID, WIDTH),
        up_weight.reshape(HID, WIDTH),
        down_weight.reshape(HID, WIDTH),
    )


def solution(mesh):
    split = Mesh(mesh.devices.reshape(ZS, SIDE, SIDE, 2), ("expert", "x", "y", "c"))
    plane = ("x", "y", "c")
    weight = P("expert", plane, None)
    in_specs = (P("expert", plane), P(), P("expert", None), P("expert", None), P("expert"), weight, weight, weight)
    return jax.shard_map(local, mesh=split, in_specs=in_specs, out_specs=P("expert", plane), check_vma=False)
```

```python
import jax
import jax.numpy as jnp
from jax import lax
from jax.experimental import pallas as pl
from jax.experimental.pallas import tpu as pltpu
from jax.sharding import Mesh
from jax.sharding import PartitionSpec as P

MESH = pl.DeviceIdType.MESH
EPS = 1e-05
ZS = 8
SIDE = 4
SEATS = 64
ROWS = ZS * SEATS
HALF = ROWS // 2
QUARTER = HALF // 2
FEAT = 128
HID = 448
WIDTH = 4096
QMAX = 32000.0

ORDER = [(0, 0), (3, 0), (1, 0), (0, 3), (0, 1), (2, 0), (3, 3), (3, 1), (1, 3), (1, 1), (0, 2), (2, 3), (2, 1), (3, 2), (1, 2), (2, 2)]
MIRROR = [ORDER.index((j, i)) for i, j in ORDER]
PRODUCTS = ((1, 3), (2, 4), (5, 10), (0, 6), (7, 8), (9, 11), (13, 12), (14, 15))
BLOCKS = ((2, 3), (1, 0))

SCHEDULE = (
    ("arr", 0, 1), ("arr", 0, 2), ("arr", 0, 4), ("arr", 0, 3), ("arr", 0, 5), ("arr", 1, 1),
    ("arr", 0, 7), ("arr", 0, 6), ("arr", 0, 9), ("arr", 0, 8), ("arr", 1, 2), ("scale", 0),
    ("arr", 0, 10), ("scale", 1), ("weights",), ("prod", 0, 0), ("arr", 1, 3), ("arr", 1, 5),
    ("prod", 0, 3), ("prod", 0, 2), ("arr", 0, 11), ("arr", 1, 4), ("prod", 0, 4), ("arr", 0, 12),
    ("prod", 0, 1), ("arr", 0, 15), ("arr", 1, 7), ("arr", 1, 6), ("arr", 0, 13), ("prod", 1, 1),
    ("arr", 0, 14), ("prod", 0, 7), ("prod", 0, 5), ("prod", 0, 6), ("hidden", 0), ("arr", 1, 12),
    ("down",), ("pre2", 0), ("arr", 1, 9), ("arr", 1, 11), ("arr", 1, 8), ("prod", 1, 0),
    ("arr", 1, 10), ("prod", 1, 3), ("p2", 0), ("ahead", 0, 0), ("ahead", 0, 1), ("prod", 1, 4),
    ("arr", 1, 15), ("pd", 0, 1), ("pd", 0, 0), ("direct", 0, 0, 1), ("arr", 1, 13), ("prod", 1, 2),
    ("direct", 0, 1, 1), ("direct", 0, 0, 0), ("arr", 1, 14), ("prod", 1, 7), ("direct", 0, 1, 0), ("p0", 0),
    ("prod", 1, 5), ("prod", 1, 6), ("hidden", 1), ("joined", 0, 0, 1), ("joined", 0, 0, 0), ("pre2", 1),
    ("joined", 0, 1, 1), ("joined", 0, 1, 0), ("p2", 1), ("ahead", 1, 0), ("p0", 1), ("ahead", 1, 1),
    ("pd", 1, 0), ("pd", 1, 1), ("direct", 1, 0, 1), ("direct", 1, 0, 0), ("direct", 1, 1, 0), ("direct", 1, 1, 1),
    ("sum", 0, 0), ("sum", 0, 1), ("sum", 0, 2), ("joined", 1, 0, 1), ("own", 0), ("joined", 1, 0, 0),
    ("joined", 1, 1, 0), ("joined", 1, 1, 1), ("finish", 0), ("sum", 1, 0), ("sum", 1, 2), ("sum", 1, 1),
    ("own", 1), ("finish", 1),
)


def encode(values, ref):
    row = lax.broadcasted_iota(jnp.int32, (16, FEAT), 0)
    scale = jnp.zeros((16, FEAT), jnp.int32)
    for n, v in enumerate(values):
        top = jnp.maximum(jnp.max(jnp.abs(v), axis=0, keepdims=True), 1e-30)
        exponent = jnp.ceil(jnp.log2(top))
        power = jnp.exp2(exponent)
        mantissa = jnp.ceil(top / power * QMAX)
        inverse = (QMAX * QMAX) / (mantissa * power)
        ref[n * QUARTER : (n + 1) * QUARTER, :] = jnp.round(v * inverse).astype(jnp.int32).astype(jnp.int16)
        scale = jnp.where(row >= 8 * n, jnp.where(row < 8 * n + 4, exponent.astype(jnp.int32), mantissa.astype(jnp.int32)), scale)
    ref[len(values) * QUARTER :, :] = scale.astype(jnp.int16)


def decode(ref, n=0):
    scale = ref[ref.shape[0] - 16 :, :].astype(jnp.int32).astype(jnp.float32)
    factor = scale[8 * n + 4 : 8 * n + 5, :] * jnp.exp2(scale[8 * n : 8 * n + 1, :]) * (1.0 / (QMAX * QMAX))
    return ref[n * QUARTER : (n + 1) * QUARTER, :].astype(jnp.int32).astype(jnp.float32) * factor


def column(row):
    return jnp.broadcast_to(row, (FEAT, FEAT)).T


def dot(a, b, dims, precision=None):
    return lax.dot_general(a, b, (dims, ((), ())), precision=precision, preferred_element_type=jnp.float32)


def kernel(
    tok_hbm, gain_hbm, logit_hbm, ids_hbm, act_hbm, wg_hbm, wu_hbm, wd_hbm, out_ref,
    tok_ref, gain_ref, logit_ref, ids_ref, act_ref,
    wide_w, dn, outbox, gathered, scale_rows, rsend, rrecv, turned, msb, xn, sums, hid, part, red,
    sfb, sdb, rfb, rdb, sda, rda, fin, ret, picks,
    w_sem, dn_sem, dns_sem, dnr_sem, z_s, z_r, rz_s, rz_r, ms_s, ms_r, g_s, g_r, d_s, d_r, h_s, h_r,
    bf_s, bf_r, bd_s, bd_r, ad_s, ad_r, t_s, t_r,
):
    z, x, y, c = (lax.axis_index(n) for n in ("expert", "x", "y", "c"))
    a = jnp.where(c == 0, x, y)
    b = jnp.where(c == 0, y, x)
    mate = {"c": 1 - c}

    def wrap(v):
        return lax.rem(v, SIDE)

    def to_a(s):
        return {"x": wrap(x + s * (1 - c)), "y": wrap(y + s * c)}

    def to_b(s):
        return {"x": wrap(x + s * c), "y": wrap(y + s * (1 - c))}

    def to_z(s):
        return {"expert": lax.rem(z + s, ZS)}

    def remote(src, dst, s_sem, r_sem, device):
        pltpu.make_async_remote_copy(src_ref=src, dst_ref=dst, send_sem=s_sem, recv_sem=r_sem, device_id=device, device_id_type=MESH).start()

    def arrived(ref, sem):
        pltpu.make_async_copy(ref, ref, sem).wait()

    def down_columns(aa, bb, core):
        xx = jnp.where(core == 0, aa, bb)
        yy = jnp.where(core == 0, bb, aa)
        return pl.ds(pl.multiple_of(((xx * SIDE + yy) * 2 + core) * FEAT, FEAT), FEAT)

    small = ((tok_hbm, tok_ref), (act_hbm, act_ref), (ids_hbm, ids_ref), (logit_hbm, logit_ref), (gain_hbm, gain_ref))
    small = [pltpu.make_async_copy(source, target, sem) for (source, target), sem in zip(small, (h_s, bf_s, bd_s, ad_s, t_s))]
    for copy in small:
        copy.start()
    barrier = pltpu.get_barrier_semaphore()
    chips = [{"x": wrap(x + n // SIDE), "y": wrap(y + n % SIDE)} for n in range(1, SIDE * SIDE)]
    peers = [mate] + chips + [to_z(s) for s in range(1, ZS)]
    for peer in peers:
        pl.semaphore_signal(barrier, inc=1, device_id=peer, device_id_type=MESH)

    for copy in small[:3]:
        copy.wait()
    for n, w in enumerate((wg_hbm, wu_hbm)):
        pltpu.make_async_copy(w, wide_w.at[n], w_sem).start()
    for aa in range(SIDE):
        for bb in range(SIDE):
            pltpu.make_async_copy(wd_hbm.at[:, down_columns(aa, bb, c)], dn.at[c, bb, :, pl.ds(aa * FEAT, FEAT)], dn_sem).start()

    tok = tok_ref[...]
    wide = tok.astype(jnp.float32)
    msb[0] = jnp.sum((wide * wide).T, axis=0, keepdims=True)

    seat_row = lax.broadcasted_iota(jnp.int32, (ROWS, FEAT), 0)
    expert_of = seat_row // SEATS
    seat_of = (seat_row - expert_of * SEATS).astype(jnp.float32)
    live = jnp.broadcast_to(act_ref[...], (ROWS, FEAT)) > 0
    first = (expert_of == jnp.broadcast_to(ids_ref[0:1, :], (ROWS, FEAT))) & live
    second = (expert_of == jnp.broadcast_to(ids_ref[1:2, :], (ROWS, FEAT))) & live
    named = jnp.where(first | second, 1.0, 0.0)
    before = jnp.where(lax.broadcasted_iota(jnp.int32, (FEAT, FEAT), 0) < lax.broadcasted_iota(jnp.int32, (FEAT, FEAT), 1), 1.0, 0.0)
    position = dot(named.astype(jnp.bfloat16), before.astype(jnp.bfloat16), ((1,), (0,)))
    seated = position == seat_of
    pick0 = jnp.where(first & seated, 1.0, 0.0)
    pick1 = jnp.where(second & seated, 1.0, 0.0)
    pick = (pick0 + pick1).astype(jnp.bfloat16)
    outbox[...] = dot(pick, tok, ((1,), (0,))).astype(jnp.bfloat16)

    picks[0] = pick0.T.astype(jnp.bfloat16)
    picks[1] = pick1.T.astype(jnp.bfloat16)
    pl.semaphore_wait(barrier, len(peers))
    remote(msb.at[0], msb.at[1], ms_s, ms_r.at[0], mate)
    me = a * SIDE + b
    my_half = z // 4
    own_seats = pl.ds(pl.multiple_of(z * SEATS, SEATS), SEATS)
    landing = gathered.at[my_half, c, me, pl.ds(pl.multiple_of(z % 4 * SEATS, SEATS), SEATS)]
    for s in (4, 5, 3, 6, 2, 7, 1):
        target = lax.rem(z + s, ZS)
        remote(outbox.at[pl.ds(pl.multiple_of(target * SEATS, SEATS), SEATS)], landing, z_s, z_r.at[my_half], to_z(s))
    pltpu.make_async_copy(outbox.at[own_seats], landing, z_r.at[my_half]).start()
    for aa in range(SIDE):
        for bb in range(SIDE):
            remote(wd_hbm.at[:, down_columns(aa, bb, 1 - c)], dn.at[c, bb, :, pl.ds(aa * FEAT, FEAT)], dns_sem, dnr_sem, mate)

    def pass_on(h, i, j, quarter, device, di, dj):
        k = wrap(a + i) * SIDE + wrap(b + j)
        ref = gathered.at[h, c, k]
        if quarter is not None:
            ref = ref.at[pl.ds(quarter * QUARTER, QUARTER)]
        remote(ref, ref, g_s, g_r.at[h, ORDER.index(((i - di) % 4, (j - dj) % 4))], device)

    def arrive(h, n):
        i, j = ORDER[n]
        k = wrap(a + i) * SIDE + wrap(b + j)
        if n == 0:
            arrived(gathered.at[h, c, k], z_r.at[h])
            pass_on(h, 0, 0, None, to_a(1), 1, 0)
            pass_on(h, 0, 0, None, to_a(3), 3, 0)
            pass_on(h, 0, 0, None, to_a(2), 2, 0)
        else:
            arrived(gathered.at[h, c, k], g_r.at[h, n])
        if j == 0:
            pass_on(h, i, j, None, to_b(1), 0, 1)
            pass_on(h, i, j, None, to_b(3), 0, 3)
        if (i, j) == (2, 0):
            pass_on(h, i, j, None, to_b(2), 0, 2)
        if j == 3 and i != 2:
            pass_on(h, i, j, 0, to_b(1), 0, 1)
        if j == 1 and i != 2:
            pass_on(h, i, j, 1, to_b(3), 0, 3)
        group = next(g for g, pair in enumerate(PRODUCTS) if MIRROR[n] in pair)
        remote(gathered.at[h, c, k], gathered.at[h, c, k], d_s, d_r.at[h, group], mate)

    opened = set()

    def product(h, group):
        arrived(gathered.at[h, 0, pl.ds(0, 2)], d_r.at[h, group])
        offsets = []
        for p, n in enumerate(PRODUCTS[group]):
            i, j = ORDER[n]
            aa, bb = wrap(a + i), wrap(b + j)
            mine, other = aa * SIDE + bb, bb * SIDE + aa
            chip = jnp.where(c == 0, mine, other)
            at = pl.ds(pl.multiple_of(chip * 2 * FEAT, 2 * FEAT), 2 * FEAT)
            gains = gain_ref[at].astype(jnp.float32).reshape(1, 2 * FEAT)
            for core in (0, 1):
                k = jnp.where(c == core, mine, other)
                lanes = slice(core * FEAT, (core + 1) * FEAT)
                normed = gathered[h, core, k].astype(jnp.float32) * scale_rows[h] * gains[:, lanes]
                xn[p, :, lanes] = normed.astype(jnp.bfloat16)
            offsets.append(at)
        for n in (0, 1):
            terms = sum(dot(wide_w[n, :, at], xn[p], ((1,), (1,))) for p, at in enumerate(offsets))
            sums[h, n] = sums[h, n] + terms if h in opened else terms
        opened.add(h)

    def hidden(h):
        g = sums[h, 0]
        hid[h, c] = (g / (1.0 + jnp.exp(-g)) * sums[h, 1]).T.astype(jnp.bfloat16)
        remote(hid.at[h, c], hid.at[h, c], h_s, h_r.at[h], mate)

    AHEAD, STEP, SIDES = 2, (1, 3), (1, 3)

    def partial(h, j, own, first):
        core = c if own else 1 - c
        terms = dot(hid[h, core], dn[core, wrap(b + j)], ((1,), (0,)))
        part[h, j] = terms if first else part[h, j] + terms

    def block(h, j, q, i):
        return part[h, j, q * QUARTER : (q + 1) * QUARTER, pl.ds(pl.multiple_of(wrap(a + i) * FEAT, FEAT), FEAT)]

    def send_ahead(h, g):
        for d in (0, 1):
            encode([block(h, AHEAD, d, i) for i in BLOCKS[g]], sfb.at[h, d, g])
            remote(sfb.at[h, d, g], rfb.at[h, d, g], bf_s, bf_r.at[h, d, g], to_b(STEP[d]))

    def send_direct(h, g, d):
        q = 1 - d
        encode([block(h, SIDES[d], q, i) for i in BLOCKS[g]], sdb.at[h, g, d, q])
        remote(sdb.at[h, g, d, q], rdb.at[h, g, d, q], bd_s, bd_r.at[h, g], to_b(STEP[d]))

    def send_joined(h, g, d):
        q = d
        arrived(rfb.at[h, d, g], bf_r.at[h, d, g])
        encode([block(h, SIDES[d], q, i) + decode(rfb.at[h, d, g], n) for n, i in enumerate(BLOCKS[g])], sdb.at[h, g, d, q])
        remote(sdb.at[h, g, d, q], rdb.at[h, g, d, q], bd_s, bd_r.at[h, g], to_b(STEP[d]))

    awaited = set()

    def summed(h, i):
        g = 0 if i in BLOCKS[0] else 1
        n = BLOCKS[g].index(i)
        if (h, g) not in awaited:
            awaited.add((h, g))
            arrived(rdb.at[h, g], bd_r.at[h, g])
        return [block(h, 0, q, i) + decode(rdb.at[h, g, 0, q], n) + decode(rdb.at[h, g, 1, q], n) for q in (0, 1)]

    def send_sum(h, n):
        i = (2, 1, 3)[n]
        encode(summed(h, i), sda.at[h, n])
        remote(sda.at[h, n], rda.at[h, n], ad_s, ad_r.at[h], to_a(i))

    def keep_sum(h):
        red[h, 0], red[h, 1] = summed(h, 0)

    def finish(h):
        arrived(rda.at[h], ad_r.at[h])
        for q in (0, 1):
            total = red[h, q] + decode(rda.at[h, 0], q) + decode(rda.at[h, 1], q) + decode(rda.at[h, 2], q)
            fin[h, q * QUARTER : (q + 1) * QUARTER, :] = total.astype(jnp.bfloat16)
        for m in range(4):
            g = h * 4 + m
            source, target = fin.at[h, pl.ds(m * SEATS, SEATS)], ret.at[own_seats]

            @pl.when(z != g)
            def _():
                remote(source, target, t_s, t_r, {"expert": g})

            @pl.when(z == g)
            def _():
                pltpu.make_async_copy(source, target, t_r).start()

    arrived(msb.at[1], ms_r.at[0])
    msb[2] = msb[0] + msb[1]
    for n, chip in enumerate(chips):
        remote(msb.at[2], msb.at[3 + n], ms_s, ms_r.at[1], chip)
    arrive(0, 0)
    arrive(1, 0)
    arrived(msb.at[pl.ds(3, 15)], ms_r.at[1])
    mean_square = jnp.sum(msb[2:18], axis=0) / WIDTH
    inverse = lax.rsqrt(mean_square + EPS)
    rsend[...] = dot(jnp.broadcast_to(inverse, (8, FEAT)), pick.astype(jnp.float32), ((1,), (1,)), lax.Precision.HIGHEST)[0:1, :]
    for s in range(1, ZS):
        remote(rsend, rrecv.at[z], rz_s, rz_r.at[my_half], to_z(s))
    pltpu.make_async_copy(rsend, rrecv.at[z], rz_r.at[my_half]).start()
    for copy in small[3:]:
        copy.wait()
    l0, l1 = logit_ref[0:1, :], logit_ref[1:2, :]
    high = jnp.maximum(l0, l1)
    e0, e1 = jnp.exp(l0 - high), jnp.exp(l1 - high)
    alive = act_ref[...].astype(jnp.float32)
    prob0 = column(e0 / (e0 + e1) * alive)
    prob1 = column(e1 / (e0 + e1) * alive)

    lane_block = pl.ds(pl.multiple_of(z // 2 * FEAT, FEAT), FEAT)
    seat_block = pl.ds(pl.multiple_of(z % 2 * SEATS, SEATS), SEATS)

    def scales(h):
        arrived(rrecv.at[pl.ds(0, 4)], rz_r.at[h])
        for m in range(4):
            turned[...] = column(rrecv[h * 4 + m, :, lane_block])
            scale_rows[h, m * SEATS : (m + 1) * SEATS, :] = turned[seat_block, :]

    def down_ready():
        arrived(dn.at[c], dn_sem)
        arrived(dn.at[1 - c], dnr_sem)

    def weights_ready():
        arrived(wide_w, w_sem)

    def both_cores(h):
        arrived(hid.at[h, 1 - c], h_r.at[h])
        partial(h, AHEAD, False, False)

    def whole_partial(h, j):
        bb = wrap(b + j)
        part[h, j] = dot(hid[h, 0], dn[0, bb], ((1,), (0,))) + dot(hid[h, 1], dn[1, bb], ((1,), (0,)))

    events = {
        "arr": arrive,
        "scale": scales,
        "weights": weights_ready,
        "prod": product,
        "hidden": hidden,
        "down": down_ready,
        "pre2": lambda h: partial(h, AHEAD, True, True),
        "p2": both_cores,
        "ahead": send_ahead,
        "pd": lambda h, d: whole_partial(h, SIDES[d]),
        "direct": send_direct,
        "joined": send_joined,
        "p0": lambda h: whole_partial(h, 0),
        "sum": send_sum,
        "own": keep_sum,
        "finish": finish,
    }
    for name, *which in SCHEDULE:
        events[name](*which)
    arrived(ret, t_r)
    back = ret[...]
    from0 = dot(picks[0], back, ((1,), (0,)))
    from1 = dot(picks[1], back, ((1,), (0,)))
    out_ref[...] = (prob0 * from0 + prob1 * from1).astype(jnp.bfloat16)

    arrived(outbox.at[pl.ds(0, ROWS - SEATS)], z_s)
    arrived(rrecv.at[pl.ds(0, ZS - 1)], rz_s)
    arrived(msb.at[pl.ds(0, 16)], ms_s)
    arrived(gathered.at[:, 0, pl.ds(0, 15)], g_s)
    arrived(gathered.at[:, 0], d_s)
    arrived(hid.at[:, 0], h_s)
    arrived(sfb, bf_s)
    arrived(sdb, bd_s)
    arrived(sda, ad_s)
    arrived(ret.at[pl.ds(0, ROWS - SEATS)], t_s)
    arrived(dn.at[c], dns_sem)


def local(tokens, norm_gain, route_logits, expert_ids, active, gate_weight, up_weight, down_weight):
    vmem = pl.BlockSpec(memory_space=pltpu.VMEM)
    hbm = pl.BlockSpec(memory_space=pltpu.HBM)
    bf16, f32, i16 = jnp.bfloat16, jnp.float32, jnp.int16
    dma = pltpu.SemaphoreType.DMA
    double = 2 * QUARTER + 16

    def pin(v):
        return pltpu.with_memory_space_constraint(v, pltpu.HBM)

    return pl.pallas_call(
        kernel,
        out_shape=jax.ShapeDtypeStruct((FEAT, FEAT), bf16),
        in_specs=[hbm] * 8,
        out_specs=vmem,
        scratch_shapes=[
            pltpu.VMEM((FEAT, FEAT), bf16),
            pltpu.VMEM((WIDTH,), bf16),
            pltpu.VMEM((2, FEAT), f32),
            pltpu.VMEM((2, FEAT), jnp.int32),
            pltpu.VMEM((1, FEAT), jnp.int32),
            pltpu.VMEM((2, HID, WIDTH), bf16),
            pltpu.VMEM((2, SIDE, HID, SIDE * FEAT), bf16),
            pltpu.VMEM((ROWS, FEAT), bf16),
            pltpu.VMEM((2, 2, 16, HALF, FEAT), bf16),
            pltpu.VMEM((2, HALF, FEAT), f32),
            pltpu.VMEM((1, ROWS), f32),
            pltpu.VMEM((ZS, 1, ROWS), f32),
            pltpu.VMEM((FEAT, FEAT), f32),
            pltpu.VMEM((18, 1, FEAT), f32),
            pltpu.VMEM((2, HALF, 2 * FEAT), bf16),
            pltpu.VMEM((2, 2, HID, HALF), f32),
            pltpu.VMEM((2, 2, HALF, HID), bf16),
            pltpu.VMEM((2, SIDE, HALF, SIDE * FEAT), f32),
            pltpu.VMEM((2, 2, QUARTER, FEAT), f32),
            pltpu.VMEM((2, 2, 2, double, FEAT), i16),
            pltpu.VMEM((2, 2, 2, 2, double, FEAT), i16),
            pltpu.VMEM((2, 2, 2, double, FEAT), i16),
            pltpu.VMEM((2, 2, 2, 2, double, FEAT), i16),
            pltpu.VMEM((2, 3, double, FEAT), i16),
            pltpu.VMEM((2, 3, double, FEAT), i16),
            pltpu.VMEM((2, HALF, FEAT), bf16),
            pltpu.VMEM((ROWS, FEAT), bf16),
            pltpu.VMEM((2, FEAT, ROWS), bf16),
            dma, dma, dma, dma,
            dma, dma((2,)), dma, dma((2,)), dma, dma((2,)),
            dma, dma((2, 16)), dma, dma((2, 8)), dma, dma((2,)),
            dma, dma((2, 2, 2)), dma, dma((2, 2)), dma, dma((2,)),
            dma, dma,
        ],
        compiler_params=pltpu.CompilerParams(collective_id=0, has_side_effects=True, vmem_limit_bytes=52 * 1024 * 1024),
    )(
        pin(tokens),
        pin(norm_gain),
        pin(route_logits.T),
        pin(expert_ids.T),
        pin(active.reshape(1, FEAT)),
        gate_weight.reshape(HID, WIDTH),
        up_weight.reshape(HID, WIDTH),
        down_weight.reshape(HID, WIDTH),
    )


def solution(mesh):
    split = Mesh(mesh.devices.reshape(ZS, SIDE, SIDE, 2), ("expert", "x", "y", "c"))
    plane = ("x", "y", "c")
    weight = P("expert", plane, None)
    in_specs = (P("expert", plane), P(), P("expert", None), P("expert", None), P("expert"), weight, weight, weight)
    return jax.shard_map(local, mesh=split, in_specs=in_specs, out_specs=P("expert", plane), check_vma=False)
```

```python
import jax
import jax.numpy as jnp
from jax import lax
from jax.experimental import pallas as pl
from jax.experimental.pallas import tpu as pltpu
from jax.sharding import Mesh
from jax.sharding import PartitionSpec as P

MESH = pl.DeviceIdType.MESH
EPS = 1e-05
ZS = 8
SIDE = 4
SEATS = 64
ROWS = ZS * SEATS
HALF = ROWS // 2
QUARTER = HALF // 2
FEAT = 128
HID = 448
WIDTH = 4096
QMAX = 32000.0

ORDER = [(0, 0), (3, 0), (1, 0), (0, 3), (0, 1), (2, 0), (3, 3), (3, 1), (1, 3), (1, 1), (0, 2), (2, 3), (2, 1), (3, 2), (1, 2), (2, 2)]
MIRROR = [ORDER.index((j, i)) for i, j in ORDER]
PRODUCTS = ((1, 3), (2, 4), (5, 10), (0, 6), (7, 8), (9, 11), (13, 12), (14, 15))
BLOCKS = ((2, 3), (1, 0))

SCHEDULE = (
    ("arr", 0, 1), ("arr", 0, 2), ("arr", 0, 4), ("arr", 0, 3), ("arr", 0, 5), ("arr", 1, 1),
    ("arr", 0, 7), ("arr", 0, 6), ("arr", 0, 9), ("arr", 0, 8), ("arr", 1, 2), ("scale", 0),
    ("arr", 0, 10), ("scale", 1), ("weights",), ("prod", 0, 0), ("arr", 1, 3), ("arr", 1, 5),
    ("prod", 0, 3), ("prod", 0, 2), ("arr", 0, 11), ("arr", 1, 4), ("prod", 0, 4), ("arr", 0, 12),
    ("prod", 0, 1), ("arr", 0, 15), ("arr", 1, 7), ("arr", 1, 6), ("arr", 0, 13), ("prod", 1, 1),
    ("arr", 0, 14), ("prod", 0, 7), ("prod", 0, 5), ("prod", 0, 6), ("hidden", 0), ("arr", 1, 12),
    ("down",), ("pre2", 0), ("arr", 1, 9), ("arr", 1, 11), ("arr", 1, 8), ("prod", 1, 0),
    ("arr", 1, 10), ("prod", 1, 3), ("p2", 0), ("ahead", 0, 0), ("ahead", 0, 1), ("prod", 1, 4),
    ("arr", 1, 15), ("pd", 0, 1), ("pd", 0, 0), ("direct", 0, 0, 1), ("direct", 0, 1, 0), ("direct", 0, 0, 0),
    ("direct", 0, 1, 1), ("arr", 1, 13), ("prod", 1, 2), ("arr", 1, 14), ("prod", 1, 7), ("p0", 0),
    ("prod", 1, 5), ("prod", 1, 6), ("hidden", 1), ("joined", 0, 0, 1), ("joined", 0, 0, 0), ("pre2", 1),
    ("joined", 0, 1, 1), ("joined", 0, 1, 0), ("p2", 1), ("ahead", 1, 0), ("ahead", 1, 1), ("pd", 1, 0),
    ("pd", 1, 1), ("direct", 1, 0, 1), ("direct", 1, 0, 0), ("direct", 1, 1, 0), ("direct", 1, 1, 1), ("p0", 1),
    ("sum", 0, 0), ("sum", 0, 1), ("sum", 0, 2), ("joined", 1, 0, 1), ("own", 0), ("joined", 1, 0, 0),
    ("joined", 1, 1, 0), ("joined", 1, 1, 1), ("finish", 0), ("sum", 1, 0), ("sum", 1, 2), ("sum", 1, 1),
    ("own", 1), ("finish", 1),
)


def encode(values, ref):
    row = lax.broadcasted_iota(jnp.int32, (16, FEAT), 0)
    scale = jnp.zeros((16, FEAT), jnp.int32)
    for n, v in enumerate(values):
        top = jnp.maximum(jnp.max(jnp.abs(v), axis=0, keepdims=True), 1e-30)
        exponent = jnp.ceil(jnp.log2(top))
        power = jnp.exp2(exponent)
        mantissa = jnp.ceil(top / power * QMAX)
        inverse = (QMAX * QMAX) / (mantissa * power)
        ref[n * QUARTER : (n + 1) * QUARTER, :] = jnp.round(v * inverse).astype(jnp.int32).astype(jnp.int16)
        scale = jnp.where(row >= 8 * n, jnp.where(row < 8 * n + 4, exponent.astype(jnp.int32), mantissa.astype(jnp.int32)), scale)
    ref[len(values) * QUARTER :, :] = scale.astype(jnp.int16)


def decode(ref, n=0):
    scale = ref[ref.shape[0] - 16 :, :].astype(jnp.int32).astype(jnp.float32)
    factor = scale[8 * n + 4 : 8 * n + 5, :] * jnp.exp2(scale[8 * n : 8 * n + 1, :]) * (1.0 / (QMAX * QMAX))
    return ref[n * QUARTER : (n + 1) * QUARTER, :].astype(jnp.int32).astype(jnp.float32) * factor


def column(row):
    return jnp.broadcast_to(row, (FEAT, FEAT)).T


def dot(a, b, dims, precision=None):
    return lax.dot_general(a, b, (dims, ((), ())), precision=precision, preferred_element_type=jnp.float32)


def kernel(
    tok_hbm, gain_hbm, logit_hbm, ids_hbm, act_hbm, wg_hbm, wu_hbm, wd_hbm, out_ref,
    tok_ref, gain_ref, logit_ref, ids_ref, act_ref,
    wide_w, dn, outbox, gathered, scale_rows, rsend, rrecv, turned, msb, xn, sums, hid, part, red,
    sfb, sdb, rfb, rdb, sda, rda, fin, ret, picks,
    w_sem, dn_sem, dns_sem, dnr_sem, z_s, z_r, rz_s, rz_r, ms_s, ms_r, g_s, g_r, d_s, d_r, h_s, h_r,
    bf_s, bf_r, bd_s, bd_r, ad_s, ad_r, t_s, t_r,
):
    z, x, y, c = (lax.axis_index(n) for n in ("expert", "x", "y", "c"))
    a = jnp.where(c == 0, x, y)
    b = jnp.where(c == 0, y, x)
    mate = {"c": 1 - c}

    def wrap(v):
        return lax.rem(v, SIDE)

    def to_a(s):
        return {"x": wrap(x + s * (1 - c)), "y": wrap(y + s * c)}

    def to_b(s):
        return {"x": wrap(x + s * c), "y": wrap(y + s * (1 - c))}

    def to_z(s):
        return {"expert": lax.rem(z + s, ZS)}

    def remote(src, dst, s_sem, r_sem, device):
        pltpu.make_async_remote_copy(src_ref=src, dst_ref=dst, send_sem=s_sem, recv_sem=r_sem, device_id=device, device_id_type=MESH).start()

    def arrived(ref, sem):
        pltpu.make_async_copy(ref, ref, sem).wait()

    def down_columns(aa, bb, core):
        xx = jnp.where(core == 0, aa, bb)
        yy = jnp.where(core == 0, bb, aa)
        return pl.ds(pl.multiple_of(((xx * SIDE + yy) * 2 + core) * FEAT, FEAT), FEAT)

    small = ((tok_hbm, tok_ref), (act_hbm, act_ref), (ids_hbm, ids_ref), (logit_hbm, logit_ref), (gain_hbm, gain_ref))
    small = [pltpu.make_async_copy(source, target, sem) for (source, target), sem in zip(small, (h_s, bf_s, bd_s, ad_s, t_s))]
    for copy in small:
        copy.start()
    barrier = pltpu.get_barrier_semaphore()
    chips = [{"x": wrap(x + n // SIDE), "y": wrap(y + n % SIDE)} for n in range(1, SIDE * SIDE)]
    peers = [mate] + chips + [to_z(s) for s in range(1, ZS)]
    for peer in peers:
        pl.semaphore_signal(barrier, inc=1, device_id=peer, device_id_type=MESH)

    for copy in small[:3]:
        copy.wait()
    for n, w in enumerate((wg_hbm, wu_hbm)):
        pltpu.make_async_copy(w, wide_w.at[n], w_sem).start()
    for aa in range(SIDE):
        for bb in range(SIDE):
            pltpu.make_async_copy(wd_hbm.at[:, down_columns(aa, bb, c)], dn.at[c, bb, :, pl.ds(aa * FEAT, FEAT)], dn_sem).start()

    tok = tok_ref[...]
    wide = tok.astype(jnp.float32)
    msb[0] = jnp.sum((wide * wide).T, axis=0, keepdims=True)

    seat_row = lax.broadcasted_iota(jnp.int32, (ROWS, FEAT), 0)
    expert_of = seat_row // SEATS
    seat_of = (seat_row - expert_of * SEATS).astype(jnp.float32)
    live = jnp.broadcast_to(act_ref[...], (ROWS, FEAT)) > 0
    first = (expert_of == jnp.broadcast_to(ids_ref[0:1, :], (ROWS, FEAT))) & live
    second = (expert_of == jnp.broadcast_to(ids_ref[1:2, :], (ROWS, FEAT))) & live
    named = jnp.where(first | second, 1.0, 0.0)
    before = jnp.where(lax.broadcasted_iota(jnp.int32, (FEAT, FEAT), 0) < lax.broadcasted_iota(jnp.int32, (FEAT, FEAT), 1), 1.0, 0.0)
    position = dot(named.astype(jnp.bfloat16), before.astype(jnp.bfloat16), ((1,), (0,)))
    seated = position == seat_of
    pick0 = jnp.where(first & seated, 1.0, 0.0)
    pick1 = jnp.where(second & seated, 1.0, 0.0)
    pick = (pick0 + pick1).astype(jnp.bfloat16)
    outbox[...] = dot(pick, tok, ((1,), (0,))).astype(jnp.bfloat16)

    picks[0] = pick0.T.astype(jnp.bfloat16)
    picks[1] = pick1.T.astype(jnp.bfloat16)
    pl.semaphore_wait(barrier, len(peers))
    remote(msb.at[0], msb.at[1], ms_s, ms_r.at[0], mate)
    me = a * SIDE + b
    my_half = z // 4
    own_seats = pl.ds(pl.multiple_of(z * SEATS, SEATS), SEATS)
    landing = gathered.at[my_half, c, me, pl.ds(pl.multiple_of(z % 4 * SEATS, SEATS), SEATS)]
    for s in (4, 5, 3, 6, 2, 7, 1):
        target = lax.rem(z + s, ZS)
        remote(outbox.at[pl.ds(pl.multiple_of(target * SEATS, SEATS), SEATS)], landing, z_s, z_r.at[my_half], to_z(s))
    pltpu.make_async_copy(outbox.at[own_seats], landing, z_r.at[my_half]).start()
    for aa in range(SIDE):
        for bb in range(SIDE):
            remote(wd_hbm.at[:, down_columns(aa, bb, 1 - c)], dn.at[c, bb, :, pl.ds(aa * FEAT, FEAT)], dns_sem, dnr_sem, mate)

    def pass_on(h, i, j, quarter, device, di, dj):
        k = wrap(a + i) * SIDE + wrap(b + j)
        ref = gathered.at[h, c, k]
        if quarter is not None:
            ref = ref.at[pl.ds(quarter * QUARTER, QUARTER)]
        remote(ref, ref, g_s, g_r.at[h, ORDER.index(((i - di) % 4, (j - dj) % 4))], device)

    def arrive(h, n):
        i, j = ORDER[n]
        k = wrap(a + i) * SIDE + wrap(b + j)
        if n == 0:
            arrived(gathered.at[h, c, k], z_r.at[h])
            pass_on(h, 0, 0, None, to_a(1), 1, 0)
            pass_on(h, 0, 0, None, to_a(3), 3, 0)
            pass_on(h, 0, 0, None, to_a(2), 2, 0)
        else:
            arrived(gathered.at[h, c, k], g_r.at[h, n])
        if j == 0:
            pass_on(h, i, j, None, to_b(1), 0, 1)
            pass_on(h, i, j, None, to_b(3), 0, 3)
        if (i, j) == (2, 0):
            pass_on(h, i, j, None, to_b(2), 0, 2)
        if j == 3 and i != 2:
            pass_on(h, i, j, 0, to_b(1), 0, 1)
        if j == 1 and i != 2:
            pass_on(h, i, j, 1, to_b(3), 0, 3)
        group = next(g for g, pair in enumerate(PRODUCTS) if MIRROR[n] in pair)
        remote(gathered.at[h, c, k], gathered.at[h, c, k], d_s, d_r.at[h, group], mate)

    opened = set()

    def product(h, group):
        arrived(gathered.at[h, 0, pl.ds(0, 2)], d_r.at[h, group])
        offsets = []
        for p, n in enumerate(PRODUCTS[group]):
            i, j = ORDER[n]
            aa, bb = wrap(a + i), wrap(b + j)
            mine, other = aa * SIDE + bb, bb * SIDE + aa
            chip = jnp.where(c == 0, mine, other)
            at = pl.ds(pl.multiple_of(chip * 2 * FEAT, 2 * FEAT), 2 * FEAT)
            gains = gain_ref[at].astype(jnp.float32).reshape(1, 2 * FEAT)
            for core in (0, 1):
                k = jnp.where(c == core, mine, other)
                lanes = slice(core * FEAT, (core + 1) * FEAT)
                normed = gathered[h, core, k].astype(jnp.float32) * scale_rows[h] * gains[:, lanes]
                xn[p, :, lanes] = normed.astype(jnp.bfloat16)
            offsets.append(at)
        for n in (0, 1):
            terms = sum(dot(wide_w[n, :, at], xn[p], ((1,), (1,))) for p, at in enumerate(offsets))
            sums[h, n] = sums[h, n] + terms if h in opened else terms
        opened.add(h)

    def hidden(h):
        g = sums[h, 0]
        hid[h, c] = (g / (1.0 + jnp.exp(-g)) * sums[h, 1]).T.astype(jnp.bfloat16)
        remote(hid.at[h, c], hid.at[h, c], h_s, h_r.at[h], mate)

    AHEAD, STEP, SIDES = 2, (1, 3), (1, 3)

    def partial(h, j, own, first):
        core = c if own else 1 - c
        terms = dot(hid[h, core], dn[core, wrap(b + j)], ((1,), (0,)))
        part[h, j] = terms if first else part[h, j] + terms

    def block(h, j, q, i):
        return part[h, j, q * QUARTER : (q + 1) * QUARTER, pl.ds(pl.multiple_of(wrap(a + i) * FEAT, FEAT), FEAT)]

    def send_ahead(h, g):
        for d in (0, 1):
            encode([block(h, AHEAD, d, i) for i in BLOCKS[g]], sfb.at[h, d, g])
            remote(sfb.at[h, d, g], rfb.at[h, d, g], bf_s, bf_r.at[h, d, g], to_b(STEP[d]))

    def send_direct(h, g, d):
        q = 1 - d
        encode([block(h, SIDES[d], q, i) for i in BLOCKS[g]], sdb.at[h, g, d, q])
        remote(sdb.at[h, g, d, q], rdb.at[h, g, d, q], bd_s, bd_r.at[h, g], to_b(STEP[d]))

    def send_joined(h, g, d):
        q = d
        arrived(rfb.at[h, d, g], bf_r.at[h, d, g])
        encode([block(h, SIDES[d], q, i) + decode(rfb.at[h, d, g], n) for n, i in enumerate(BLOCKS[g])], sdb.at[h, g, d, q])
        remote(sdb.at[h, g, d, q], rdb.at[h, g, d, q], bd_s, bd_r.at[h, g], to_b(STEP[d]))

    awaited = set()

    def summed(h, i):
        g = 0 if i in BLOCKS[0] else 1
        n = BLOCKS[g].index(i)
        if (h, g) not in awaited:
            awaited.add((h, g))
            arrived(rdb.at[h, g], bd_r.at[h, g])
        return [block(h, 0, q, i) + decode(rdb.at[h, g, 0, q], n) + decode(rdb.at[h, g, 1, q], n) for q in (0, 1)]

    def send_sum(h, n):
        i = (2, 1, 3)[n]
        encode(summed(h, i), sda.at[h, n])
        remote(sda.at[h, n], rda.at[h, n], ad_s, ad_r.at[h], to_a(i))

    def keep_sum(h):
        red[h, 0], red[h, 1] = summed(h, 0)

    def finish(h):
        arrived(rda.at[h], ad_r.at[h])
        for q in (0, 1):
            total = red[h, q] + decode(rda.at[h, 0], q) + decode(rda.at[h, 1], q) + decode(rda.at[h, 2], q)
            fin[h, q * QUARTER : (q + 1) * QUARTER, :] = total.astype(jnp.bfloat16)
        for m in range(4):
            g = h * 4 + m
            source, target = fin.at[h, pl.ds(m * SEATS, SEATS)], ret.at[own_seats]

            @pl.when(z != g)
            def _():
                remote(source, target, t_s, t_r, {"expert": g})

            @pl.when(z == g)
            def _():
                pltpu.make_async_copy(source, target, t_r).start()

    arrived(msb.at[1], ms_r.at[0])
    msb[2] = msb[0] + msb[1]
    for n, chip in enumerate(chips):
        remote(msb.at[2], msb.at[3 + n], ms_s, ms_r.at[1], chip)
    arrive(0, 0)
    arrive(1, 0)
    arrived(msb.at[pl.ds(3, 15)], ms_r.at[1])
    mean_square = jnp.sum(msb[2:18], axis=0) / WIDTH
    inverse = lax.rsqrt(mean_square + EPS)
    rsend[...] = dot(jnp.broadcast_to(inverse, (8, FEAT)), pick.astype(jnp.float32), ((1,), (1,)), lax.Precision.HIGHEST)[0:1, :]
    for s in range(1, ZS):
        remote(rsend, rrecv.at[z], rz_s, rz_r.at[my_half], to_z(s))
    pltpu.make_async_copy(rsend, rrecv.at[z], rz_r.at[my_half]).start()
    for copy in small[3:]:
        copy.wait()
    l0, l1 = logit_ref[0:1, :], logit_ref[1:2, :]
    high = jnp.maximum(l0, l1)
    e0, e1 = jnp.exp(l0 - high), jnp.exp(l1 - high)
    alive = act_ref[...].astype(jnp.float32)
    prob0 = column(e0 / (e0 + e1) * alive)
    prob1 = column(e1 / (e0 + e1) * alive)

    lane_block = pl.ds(pl.multiple_of(z // 2 * FEAT, FEAT), FEAT)
    seat_block = pl.ds(pl.multiple_of(z % 2 * SEATS, SEATS), SEATS)

    def scales(h):
        arrived(rrecv.at[pl.ds(0, 4)], rz_r.at[h])
        for m in range(4):
            turned[...] = column(rrecv[h * 4 + m, :, lane_block])
            scale_rows[h, m * SEATS : (m + 1) * SEATS, :] = turned[seat_block, :]

    def down_ready():
        arrived(dn.at[c], dn_sem)
        arrived(dn.at[1 - c], dnr_sem)

    def weights_ready():
        arrived(wide_w, w_sem)

    def both_cores(h):
        arrived(hid.at[h, 1 - c], h_r.at[h])
        partial(h, AHEAD, False, False)

    def whole_partial(h, j):
        bb = wrap(b + j)
        part[h, j] = dot(hid[h, 0], dn[0, bb], ((1,), (0,))) + dot(hid[h, 1], dn[1, bb], ((1,), (0,)))

    events = {
        "arr": arrive,
        "scale": scales,
        "weights": weights_ready,
        "prod": product,
        "hidden": hidden,
        "down": down_ready,
        "pre2": lambda h: partial(h, AHEAD, True, True),
        "p2": both_cores,
        "ahead": send_ahead,
        "pd": lambda h, d: whole_partial(h, SIDES[d]),
        "direct": send_direct,
        "joined": send_joined,
        "p0": lambda h: whole_partial(h, 0),
        "sum": send_sum,
        "own": keep_sum,
        "finish": finish,
    }
    for name, *which in SCHEDULE:
        events[name](*which)
    arrived(ret, t_r)
    back = ret[...]
    from0 = dot(picks[0], back, ((1,), (0,)))
    from1 = dot(picks[1], back, ((1,), (0,)))
    out_ref[...] = (prob0 * from0 + prob1 * from1).astype(jnp.bfloat16)

    arrived(outbox.at[pl.ds(0, ROWS - SEATS)], z_s)
    arrived(rrecv.at[pl.ds(0, ZS - 1)], rz_s)
    arrived(msb.at[pl.ds(0, 16)], ms_s)
    arrived(gathered.at[:, 0, pl.ds(0, 15)], g_s)
    arrived(gathered.at[:, 0], d_s)
    arrived(hid.at[:, 0], h_s)
    arrived(sfb, bf_s)
    arrived(sdb, bd_s)
    arrived(sda, ad_s)
    arrived(ret.at[pl.ds(0, ROWS - SEATS)], t_s)
    arrived(dn.at[c], dns_sem)


def local(tokens, norm_gain, route_logits, expert_ids, active, gate_weight, up_weight, down_weight):
    vmem = pl.BlockSpec(memory_space=pltpu.VMEM)
    hbm = pl.BlockSpec(memory_space=pltpu.HBM)
    bf16, f32, i16 = jnp.bfloat16, jnp.float32, jnp.int16
    dma = pltpu.SemaphoreType.DMA
    double = 2 * QUARTER + 16

    def pin(v):
        return pltpu.with_memory_space_constraint(v, pltpu.HBM)

    return pl.pallas_call(
        kernel,
        out_shape=jax.ShapeDtypeStruct((FEAT, FEAT), bf16),
        in_specs=[hbm] * 8,
        out_specs=vmem,
        scratch_shapes=[
            pltpu.VMEM((FEAT, FEAT), bf16),
            pltpu.VMEM((WIDTH,), bf16),
            pltpu.VMEM((2, FEAT), f32),
            pltpu.VMEM((2, FEAT), jnp.int32),
            pltpu.VMEM((1, FEAT), jnp.int32),
            pltpu.VMEM((2, HID, WIDTH), bf16),
            pltpu.VMEM((2, SIDE, HID, SIDE * FEAT), bf16),
            pltpu.VMEM((ROWS, FEAT), bf16),
            pltpu.VMEM((2, 2, 16, HALF, FEAT), bf16),
            pltpu.VMEM((2, HALF, FEAT), f32),
            pltpu.VMEM((1, ROWS), f32),
            pltpu.VMEM((ZS, 1, ROWS), f32),
            pltpu.VMEM((FEAT, FEAT), f32),
            pltpu.VMEM((18, 1, FEAT), f32),
            pltpu.VMEM((2, HALF, 2 * FEAT), bf16),
            pltpu.VMEM((2, 2, HID, HALF), f32),
            pltpu.VMEM((2, 2, HALF, HID), bf16),
            pltpu.VMEM((2, SIDE, HALF, SIDE * FEAT), f32),
            pltpu.VMEM((2, 2, QUARTER, FEAT), f32),
            pltpu.VMEM((2, 2, 2, double, FEAT), i16),
            pltpu.VMEM((2, 2, 2, 2, double, FEAT), i16),
            pltpu.VMEM((2, 2, 2, double, FEAT), i16),
            pltpu.VMEM((2, 2, 2, 2, double, FEAT), i16),
            pltpu.VMEM((2, 3, double, FEAT), i16),
            pltpu.VMEM((2, 3, double, FEAT), i16),
            pltpu.VMEM((2, HALF, FEAT), bf16),
            pltpu.VMEM((ROWS, FEAT), bf16),
            pltpu.VMEM((2, FEAT, ROWS), bf16),
            dma, dma, dma, dma,
            dma, dma((2,)), dma, dma((2,)), dma, dma((2,)),
            dma, dma((2, 16)), dma, dma((2, 8)), dma, dma((2,)),
            dma, dma((2, 2, 2)), dma, dma((2, 2)), dma, dma((2,)),
            dma, dma,
        ],
        compiler_params=pltpu.CompilerParams(collective_id=0, has_side_effects=True, vmem_limit_bytes=52 * 1024 * 1024),
    )(
        pin(tokens),
        pin(norm_gain),
        pin(route_logits.T),
        pin(expert_ids.T),
        pin(active.reshape(1, FEAT)),
        gate_weight.reshape(HID, WIDTH),
        up_weight.reshape(HID, WIDTH),
        down_weight.reshape(HID, WIDTH),
    )


def solution(mesh):
    split = Mesh(mesh.devices.reshape(ZS, SIDE, SIDE, 2), ("expert", "x", "y", "c"))
    plane = ("x", "y", "c")
    weight = P("expert", plane, None)
    in_specs = (P("expert", plane), P(), P("expert", None), P("expert", None), P("expert"), weight, weight, weight)
    return jax.shard_map(local, mesh=split, in_specs=in_specs, out_specs=P("expert", plane), check_vma=False)
```
